128 devices in a mesh: rows: 32 (over y, z, core), rhs: 4 (over x).
Axes of the slice: x: 4, y: 4, z: 4, core: 2. Of those that a mesh axis runs over, the one named last changes fastest.
Arguments:
- upper_unit: float32 [512, 128, 128], P('rows'), may hold values from -1 to 1, as said below
- lower_unit: float32 [512, 128, 128], P('rows'), may hold values from -1 to 1, as said below
- pivot_inv: float32 [512, 128, 128], P('rows'), may hold values from -0.25 to 2.25
- loss_grad_one: float32 [512, 128, 128], P('rows', 'rhs'), may hold values from -6 to 6
- loss_grad_two: float32 [512, 128, 128], P('rows', 'rhs'), may hold values from -0.046875 to 0.046875
- state_one: float32 [512, 128, 128], P('rows', 'rhs'), may hold values from -0.0029296875 to 0.0029296875
- state_two: float32 [512, 128, 128], P('rows', 'rhs'), may hold values from -1.5 to 1.5
Outputs:
- operator_grad: float32 [128, 3, 512, 128], P('rhs', None, 'rows')
The draws below stay inside these ranges and needn't reach their ends.
Inputs may be any that keep to these rules, and one draw needn't show every extreme that they name: `upper_unit`: every block has spectral norm below 1. `lower_unit`: every block has spectral norm below 1.
All inputs are finite; a program needn't handle non-finite values.
Results may differ from the reference program's by a relative error of at most 0.0003.
Values sent between devices are 32-bit elements; how exact they have to be, the bound alone decides.
A program may use at most 128 MiB of HBM per device.

```python
import math
import jax
import jax.numpy as jnp
from jax import lax

CELL_COMPONENTS = 128
DIRECTIONS = 128
TOTAL_BLOCK_ROWS = 512


EXACT_ARITHMETIC = lax.Precision.HIGHEST


def chain_factors(key, salt_value):
    salted = jax.random.fold_in(key, salt_value)
    random_subkeys = jax.random.split(salted, 8)
    reference_frame_basis = jnp.linalg.qr(jax.random.normal(random_subkeys[0], (CELL_COMPONENTS, CELL_COMPONENTS), jnp.float32))[0]
    slow_count = CELL_COMPONENTS // 2
    shuffled = jax.random.permutation(random_subkeys[1], CELL_COMPONENTS)
    slow_row_mask = shuffled < slow_count
    same_group = (slow_row_mask[:, None] == slow_row_mask[None, :]).astype(jnp.float32)
    group_weight = same_group + 0.03 * (1.0 - same_group)
    mixing = jax.random.normal(random_subkeys[2], (TOTAL_BLOCK_ROWS, CELL_COMPONENTS, CELL_COMPONENTS), jnp.float32) * group_weight
    rotation = jnp.linalg.qr(mixing)[0]
    fast_rate = jnp.exp(jax.random.uniform(random_subkeys[3], (CELL_COMPONENTS,), jnp.float32, math.log(0.0005), math.log(0.2)))
    slow_rate = math.log(10.0) / (4.0 * TOTAL_BLOCK_ROWS)
    base_rate = jnp.where(slow_row_mask, slow_rate, fast_rate)
    diagonal_nudge = jnp.exp(jax.random.uniform(random_subkeys[4], (TOTAL_BLOCK_ROWS, CELL_COMPONENTS), jnp.float32, math.log(0.5), math.log(2.0)))
    damping_multiplier = jnp.exp(-base_rate[None, :] * diagonal_nudge)
    spike_row_indices = jax.random.randint(random_subkeys[5], (3,), 0, TOTAL_BLOCK_ROWS)
    spike_row_mask = jnp.any(jnp.arange(TOTAL_BLOCK_ROWS)[:, None] == spike_row_indices[None, :], axis=1)
    spike_keep_flags = jax.random.uniform(random_subkeys[6], (TOTAL_BLOCK_ROWS, CELL_COMPONENTS), jnp.float32, 0.5, 0.8)
    damping_multiplier = damping_multiplier * jnp.where(spike_row_mask[:, None] & slow_row_mask[None, :], spike_keep_flags, 1.0)
    scaled_result = damping_multiplier[:, :, None] * rotation
    return jnp.einsum('jr,erf,lf->ejl', reference_frame_basis, scaled_result, reference_frame_basis, precision=EXACT_ARITHMETIC)


def draw_upper_unit(key, part):
    return chain_factors(key, 11)


def draw_lower_unit(key, part):
    return chain_factors(key, 23)


def draw_pivot_inv(key, part):
    salted = jax.random.fold_in(key, 37)
    random_subkeys = jax.random.split(salted, 2)
    diagonal = jnp.exp(jax.random.uniform(random_subkeys[0], (TOTAL_BLOCK_ROWS, CELL_COMPONENTS), jnp.float32, math.log(0.5), math.log(2.0)))
    perturb = jnp.clip(jax.random.normal(random_subkeys[1], (TOTAL_BLOCK_ROWS, CELL_COMPONENTS, CELL_COMPONENTS), jnp.float32), -4.0, 4.0)
    perturb = perturb * (0.3 / math.sqrt(CELL_COMPONENTS))
    return perturb + diagonal[:, :, None] * jnp.eye(CELL_COMPONENTS, dtype=jnp.float32)


def block_scale(stream_key, shape, cuts, low, high):
    def one(dim, parts):
        draws = jax.random.uniform(jax.random.fold_in(jax.random.fold_in(stream_key, 6), dim), (parts,), jnp.float32, low / len(cuts), high / len(cuts))
        return jnp.repeat(jnp.exp(draws), shape[dim] // parts).reshape((-1,) + (1,) * (len(shape) - dim - 1))

    factor_of = one(*cuts[0])
    for cut in cuts[1:]:
        factor_of = factor_of * one(*cut)
    return factor_of


def gaussian(key, shape, spread, limit, cuts=(), kind=jnp.bfloat16):
    values = jax.random.normal(key, shape, jnp.float32) * spread
    if len(cuts) > 0:
        values = block_scale(key, shape, cuts, -0.22, 0.18) * values
    return jnp.clip(values, min=-limit, max=limit).astype(kind)


def setup_inputs(seed: int = 0) -> dict:
    arg_keys = jax.random.split(jax.random.key(seed), 8)
    return {
        "upper_unit": draw_upper_unit(jax.random.fold_in(arg_keys[7], 71), 0),
        "lower_unit": draw_lower_unit(jax.random.fold_in(arg_keys[7], 71), 0),
        "pivot_inv": draw_pivot_inv(jax.random.fold_in(arg_keys[7], 71), 0),
        "loss_grad_one": gaussian(arg_keys[3], (TOTAL_BLOCK_ROWS, DIRECTIONS, CELL_COMPONENTS), 1.0, 6.0, ((0, 32), (1, 4)), jnp.float32),
        "loss_grad_two": gaussian(arg_keys[4], (TOTAL_BLOCK_ROWS, DIRECTIONS, CELL_COMPONENTS), (1.5 / TOTAL_BLOCK_ROWS), 0.046875, ((0, 32), (1, 4)), jnp.float32),
        "state_one": gaussian(arg_keys[5], (TOTAL_BLOCK_ROWS, DIRECTIONS, CELL_COMPONENTS), (0.1 / TOTAL_BLOCK_ROWS), 0.0029296875, ((0, 32), (1, 4)), jnp.float32),
        "state_two": gaussian(arg_keys[6], (TOTAL_BLOCK_ROWS, DIRECTIONS, CELL_COMPONENTS), 0.1, 1.5, ((0, 32), (1, 4)), jnp.float32),
    }


EXACT_ARITHMETIC = lax.Precision.HIGHEST

def advance(carried, element):
    source_row, factor = element
    solved = source_row - carried
    return (jnp.dot(solved, factor, precision=EXACT_ARITHMETIC), solved)

def transposed_solve(right_side, upper_unit, lower_unit, pivot_inv):
    initial = jnp.zeros(right_side.shape[1:], jnp.float32)
    _, lifted = lax.scan(advance, initial, (right_side, upper_unit))
    scaled_result = jnp.einsum('irb,ibc->irc', lifted, pivot_inv, precision=EXACT_ARITHMETIC)
    _, result = lax.scan(advance, initial, (scaled_result, lower_unit), reverse=True)
    return result

def outer_sum(adjoint, stored):
    return jnp.einsum('ira,irb->aib', adjoint, stored, precision=EXACT_ARITHMETIC)

def reference(upper_unit, lower_unit, pivot_inv, loss_grad_one, loss_grad_two, state_one, state_two):
    adjoint_two = transposed_solve(loss_grad_two, upper_unit, lower_unit, pivot_inv)
    adjoint_one = transposed_solve(loss_grad_one + adjoint_two, upper_unit, lower_unit, pivot_inv)
    zero_row = jnp.zeros_like(state_one[:1])
    variants = ((state_one, state_two), (jnp.concatenate([zero_row, state_one[:-1]], axis=0), jnp.concatenate([zero_row, state_two[:-1]], axis=0)), (jnp.concatenate([state_one[1:], zero_row], axis=0), jnp.concatenate([state_two[1:], zero_row], axis=0)))
    pieces = []
    for solution_past_opening, solution_past_closing in variants:
        pieces.append(outer_sum(adjoint_one, solution_past_opening) + outer_sum(adjoint_two, solution_past_closing))
    return -jnp.stack(pieces, axis=1)
```

```python
import jax
import jax.numpy as jnp
from jax import lax
from jax.experimental import pallas as pl
from jax.experimental.pallas import tpu as pltpu
from jax.sharding import PartitionSpec as P

MESH = pl.DeviceIdType.MESH
F32, BF16 = jnp.float32, jnp.bfloat16
N = 16
W = 128
R = 32
EM, EN, EK, EF, EH, ES = 0, 128, 256, 384, 416, 448


def split(x):
    hi = x.astype(BF16)
    lo = (x - hi.astype(F32)).astype(BF16)
    return hi, lo


def tile_of(w):
    hi, lo = split(w)
    row = jnp.concatenate([hi, lo], axis=1)
    return jnp.concatenate([row, row], axis=0)


def mm(x, tile):
    hi, lo = split(x)
    both = jnp.concatenate([hi, lo], axis=1)
    out = jnp.dot(both, tile, preferred_element_type=F32)
    return out[:, :W] + out[:, W:]


def mm_pair(a, l, tile):
    ah, al = split(a)
    lh, ll = split(l)
    hi = jnp.concatenate([ah, lh], axis=1)
    lo = jnp.concatenate([al, ll], axis=1)
    out = jnp.dot(jnp.concatenate([hi, lo], axis=0), tile, preferred_element_type=F32)
    m = a.shape[0]
    out = out[:m] + out[m:]
    return out[:, :W] + out[:, W:]


def kernel(
    u_ref, l_ref, p_ref, g1_ref, g2_ref, s1_ref, s2_ref, out_ref,
    tu, tp, tl, tab, zs, v2, v1,
    g_c, g_z, g_y, t_c, t_z, t_y, h_c, h_z, h_y, r_c, r_z, ae, le,
    sg, halo, ss, ps, pr, lt,
    sem_c, sem_z, sem_y, sem_hc, sem_hz, sem_hy, sem_s, sem_own, sem_halo, sem_p,
):
    d = lax.axis_index("rows")
    x = lax.axis_index("rhs")
    y, z, c = d // 8, (d // 2) % 4, d % 2

    def in_c(j):
        return (y * 8 + z * 2 + (c + j) % 2, x)

    def in_z(j):
        return (y * 8 + ((z + j) % 4) * 2 + c, x)

    def in_y(j):
        return (((y + j) % 4) * 8 + z * 2 + c, x)

    def in_x(j):
        return (d, (x + j) % 4)

    after, before = ((d + 1) % 32, x), ((d + 31) % 32, x)

    barrier = pltpu.get_barrier_semaphore()
    peers = [in_c(1)] + [f(j) for f in (in_z, in_y, in_x) for j in (1, 2, 3)] + [after, before]
    for peer in peers:
        pl.semaphore_signal(barrier, inc=1, device_id=peer, device_id_type=MESH)
    pl.semaphore_wait(barrier, len(peers))

    own = [
        pltpu.make_async_copy(s, sg.at[x, t], sem_own.at[t]) for t, s in enumerate((s1_ref, s2_ref))
    ]
    for copy in own:
        copy.start()
    for copy in own:
        copy.wait()
    states = [
        pltpu.make_async_remote_copy(
            src_ref=sg.at[x], dst_ref=sg.at[x],
            send_sem=sem_s.at[0, j - 1], recv_sem=sem_s.at[1, j - 1],
            device_id=in_x(j), device_id_type=MESH,
        )
        for j in (1, 3, 2)
    ]
    for copy in states:
        copy.start()

    def spread(ref, me, size, where, sem):
        copies = [
            pltpu.make_async_remote_copy(
                src_ref=ref.at[me], dst_ref=ref.at[me],
                send_sem=sem.at[0, j - 1], recv_sem=sem.at[1, j - 1],
                device_id=where(j), device_id_type=MESH,
            )
            for j in range(1, size)
        ]
        for copy in copies:
            copy.start()
        return copies

    def finish(copies):
        for copy in copies:
            copy.wait()

    eye = (
        lax.broadcasted_iota(jnp.int32, (W, W), 0) == lax.broadcasted_iota(jnp.int32, (W, W), 1)
    ).astype(F32)
    zero_m = jnp.zeros((W, W), F32)
    zero_v = jnp.zeros((R, W), F32)

    def up_first(i, carry):
        tile = tile_of(u_ref[i])
        tu[i] = tile
        tile_p = tile_of(p_ref[i])
        tp[i] = tile_p
        yv = jnp.concatenate([g2_ref[i], zero_m], axis=0) - carry
        zs[i] = mm(yv, tile_p)
        return mm(yv, tile)

    carry = lax.fori_loop(0, N, up_first, jnp.concatenate([zero_v, eye], axis=0))
    g_c[c, EF:EH] = carry[:R]
    g_c[c, EM:EN] = carry[R:]

    def down_first(k, carry):
        i = N - 1 - k
        tile = tile_of(l_ref[i])
        tl[i] = tile
        vv = jnp.concatenate([zs[i], zero_m], axis=0) - carry
        v2[i] = vv[:R]
        hi, lo = split(vv[R:])
        tab[i] = jnp.concatenate([hi, lo], axis=1)
        return mm(vv, tile)

    carry = lax.fori_loop(0, N, down_first, jnp.concatenate([zero_v, zero_m, eye], axis=0))
    g_c[c, EH:ES] = carry[:R]
    g_c[c, EN:EK] = carry[R : R + W]
    g_c[c, EK:EF] = carry[R + W :]

    def gather_first(g, t, me, size, where, sem):
        copies = spread(g, me, size, where, sem)
        finish(copies)
        for e in range(size):
            for m in range(3):
                t[e, m] = tile_of(g[e, m * W : (m + 1) * W])

    def level_maps(g, t, r, me, size):
        a = jnp.concatenate([zero_v, eye], axis=0)
        many = []
        for e in range(size):
            ae[e] = a
            many.append(a)
            a = mm(a, t[e, 0]) + jnp.concatenate([g[e, EF:EH], zero_m], axis=0)
        l = jnp.concatenate([zero_v, zero_m, eye], axis=0)
        for e in reversed(range(size)):
            le[e] = l
            source = jnp.concatenate([g[e, EH:ES], zero_m], axis=0) + mm(many[e], t[e, 1])
            l = mm(l, t[e, 2]) + jnp.concatenate([source, zero_m], axis=0)
        r[0] = tile_of(ae[me, R:])
        r[1] = tile_of(le[me, R : R + W])
        r[2] = tile_of(le[me, R + W :])
        return (a, l), (ae[me, :R], le[me, :R])

    def level(vec, t, me, size):
        a = zero_v
        many = []
        for e in range(size):
            ae[e, :R] = a
            many.append(a)
            a = mm(a, t[e, 0]) + vec(e, 0)
        l = zero_v
        for e in reversed(range(size)):
            le[e, :R] = l
            l = mm(l, t[e, 2]) + (vec(e, 1) + mm(many[e], t[e, 1]))
        return (a, l), (ae[me, :R], le[me, :R])

    def put(g, me, a, l):
        g[me, EF:EH] = a[:R]
        g[me, EM:EN] = a[R:]
        g[me, EH:ES] = l[:R]
        g[me, EN:EK] = l[R : R + W]
        g[me, EK:EF] = l[R + W :]

    def enter(inside, r, a, l):
        return inside[0] + mm(a, r[0]), inside[1] + mm(a, r[1]) + mm(l, r[2])

    def vec_of(g):
        return lambda e, side: g[e, EF + R * side : EF + R * side + R]

    def vec_small(h):
        return lambda e, side: h[e, R * side : R * side + R]

    gather_first(g_c, t_c, c, 2, in_c, sem_c)
    total, inside_c = level_maps(g_c, t_c, r_c, c, 2)
    put(g_z, z, *total)
    gather_first(g_z, t_z, z, 4, in_z, sem_z)
    total, inside_z = level_maps(g_z, t_z, r_z, z, 4)
    put(g_y, y, *total)
    gather_first(g_y, t_y, y, 4, in_y, sem_y)
    _, (a, l) = level(vec_of(g_y), t_y, y, 4)
    a, l = enter(inside_z, r_z, a, l)
    a, l = enter(inside_c, r_c, a, l)

    def settle(v, a, l):
        def one(i, none):
            v[i] = v[i] + mm_pair(a, l, tab[i])
            return none

        lax.fori_loop(0, N, one, 0)

    settle(v2, a, l)

    block_of = lax.broadcasted_iota(jnp.int32, (W, W), 1) // R

    def share(v, t):
        groups = [v[4 * q : 4 * q + 4].reshape(W, W) for q in range(4)]
        for dest in range(4):
            piece = groups[dest]
            for q in range(4):
                if q != dest:
                    moved = pltpu.roll(groups[q], (R * (q - dest)) % W, 1)
                    piece = jnp.where(block_of == q, moved, piece)
            if True:
                own_q = groups[dest]
                piece = jnp.where(block_of == dest, own_q, piece)
            ps[t, dest] = piece
        pr[t, x] = ps[t, x]
        copies = [
            pltpu.make_async_remote_copy(
                src_ref=ps.at[t, (x + j) % 4], dst_ref=pr.at[t, x],
                send_sem=sem_p.at[t, 0, j - 1], recv_sem=sem_p.at[t, 1, j - 1],
                device_id=in_x(j), device_id_type=MESH,
            )
            for j in (1, 3, 2)
        ]
        for copy in copies:
            copy.start()
        return copies

    shared_two = share(v2, 1)

    def up(i, carry):
        yv = g1_ref[i] + v2[i] - carry
        zs[i, :R] = mm(yv, tp[i])
        return mm(yv, tu[i])

    h_c[c, :R] = lax.fori_loop(0, N, up, zero_v)

    def down(k, carry):
        i = N - 1 - k
        vv = zs[i, :R] - carry
        v1[i] = vv
        return mm(vv, tl[i])

    h_c[c, R:] = lax.fori_loop(0, N, down, zero_v)

    finish(spread(h_c, c, 2, in_c, sem_hc))
    (a, l), inside_c = level(vec_small(h_c), t_c, c, 2)
    h_z[z, :R] = a
    h_z[z, R:] = l
    in_flight = spread(h_z, z, 4, in_z, sem_hz)

    finish(states)
    edges = []
    for side, (row, where) in enumerate(((N - 1, after), (0, before))):
        for q in range(4):
            copy = pltpu.make_async_remote_copy(
                src_ref=sg.at[q, :, row], dst_ref=halo.at[side, q],
                send_sem=sem_halo.at[0, side, q], recv_sem=sem_halo.at[1, side, q],
                device_id=where, device_id_type=MESH,
            )
            copy.start()
            edges.append(copy)

    def operand(parts):
        hi, lo = split(jnp.concatenate(parts, axis=0))
        return jnp.concatenate([hi, lo], axis=1)

    def pack(i, none):
        ss[i + 1] = operand([sg[q, t, i] for t in range(2) for q in range(4)])
        return none

    lax.fori_loop(0, N, pack, 0)

    finish(in_flight)
    (a, l), inside_z = level(vec_small(h_z), t_z, z, 4)
    h_y[y, :R] = a
    h_y[y, R:] = l
    in_flight = spread(h_y, y, 4, in_y, sem_hy)

    finish(edges)
    keep = ((d > 0).astype(F32), (d < 31).astype(F32))
    for side, slot in ((0, 0), (1, N + 1)):
        ss[slot] = operand([halo[side, q, t] * keep[side] for t in range(2) for q in range(4)])

    finish(in_flight)
    _, (a, l) = level(vec_small(h_y), t_y, y, 4)
    a, l = enter(inside_z, r_z, a, l)
    a, l = enter(inside_c, r_c, a, l)
    settle(v1, a, l)
    finish(shared_two)
    shared_one = share(v1, 0)

    def turn(t):
        for sub in range(4):
            stack = jnp.concatenate(
                [pr[t, q, R * sub : R * sub + R] for q in range(4)], axis=0
            ).T
            hi, lo = split(stack)
            for q in range(4):
                lt[4 * q + sub, :R, t * W : (t + 1) * W] = hi[R * q : R * q + R]
                lt[4 * q + sub, R:, t * W : (t + 1) * W] = lo[R * q : R * q + R]

    turn(1)
    finish(shared_one)
    turn(0)

    def grads(i, none):
        for k, j in enumerate((1, 0, 2)):
            o = jnp.dot(lt[i], ss[i + j], preferred_element_type=F32)
            o = o[:R] + o[R:]
            out_ref[k, i] = -(o[:, :W] + o[:, W:])
        return none

    lax.fori_loop(0, N, grads, 0)


def body(upper_unit, lower_unit, pivot_inv, loss_grad_one, loss_grad_two, state_one, state_two):
    vmem = pl.BlockSpec(memory_space=pltpu.VMEM)
    anywhere = pl.BlockSpec(memory_space=pl.ANY)
    dma = pltpu.SemaphoreType.DMA
    tile = (2 * W, 2 * W)
    grads = pl.pallas_call(
        kernel,
        out_shape=jax.ShapeDtypeStruct((3, N, R, W), F32),
        in_specs=[vmem] * 5 + [anywhere] * 2,
        out_specs=vmem,
        scratch_shapes=[
            pltpu.VMEM((N, *tile), BF16),
            pltpu.VMEM((N, *tile), BF16),
            pltpu.VMEM((N, *tile), BF16),
            pltpu.VMEM((N, *tile), BF16),
            pltpu.VMEM((N, R + W, W), F32),
            pltpu.VMEM((N, R, W), F32),
            pltpu.VMEM((N, R, W), F32),
            pltpu.VMEM((2, ES, W), F32),
            pltpu.VMEM((4, ES, W), F32),
            pltpu.VMEM((4, ES, W), F32),
            pltpu.VMEM((2, 3, *tile), BF16),
            pltpu.VMEM((4, 3, *tile), BF16),
            pltpu.VMEM((4, 3, *tile), BF16),
            pltpu.VMEM((2, 2 * R, W), F32),
            pltpu.VMEM((4, 2 * R, W), F32),
            pltpu.VMEM((4, 2 * R, W), F32),
            pltpu.VMEM((3, *tile), BF16),
            pltpu.VMEM((3, *tile), BF16),
            pltpu.VMEM((4, R + W, W), F32),
            pltpu.VMEM((4, R + 2 * W, W), F32),
            pltpu.VMEM((4, 2, N, R, W), F32),
            pltpu.VMEM((2, 4, 2, R, W), F32),
            pltpu.VMEM((N + 2, *tile), BF16),
            pltpu.VMEM((2, 4, W, W), F32),
            pltpu.VMEM((2, 4, W, W), F32),
            pltpu.VMEM((N, 2 * R, 2 * W), BF16),
            dma((2, 1)), dma((2, 3)), dma((2, 3)),
            dma((2, 1)), dma((2, 3)), dma((2, 3)),
            dma((2, 3)), dma((2,)), dma((2, 2, 4)), dma((2, 2, 3)),
        ],
        compiler_params=pltpu.CompilerParams(
            collective_id=0, has_side_effects=True, vmem_limit_bytes=60 * 2**20
        ),
    )(upper_unit, lower_unit, pivot_inv, loss_grad_one, loss_grad_two, state_one, state_two)
    return jnp.transpose(grads, (2, 0, 1, 3))


def solution(mesh):
    by_rows = P("rows", None, None)
    by_both = P("rows", "rhs", None)
    return jax.shard_map(
        body,
        mesh=mesh,
        in_specs=(by_rows,) * 3 + (by_both,) * 4,
        out_specs=P("rhs", None, "rows", None),
        check_vma=False,
    )
```

```python
import jax
import jax.numpy as jnp
from jax import lax
from jax.experimental import pallas as pl
from jax.experimental.pallas import tpu as pltpu
from jax.sharding import PartitionSpec as P

MESH = pl.DeviceIdType.MESH
F32, BF16 = jnp.float32, jnp.bfloat16
N = 16
W = 128
R = 32
EM, EN, EK, EF, EH, ES = 0, 128, 256, 384, 416, 448


def split(x):
    hi = x.astype(BF16)
    lo = (x - hi.astype(F32)).astype(BF16)
    return hi, lo


def tile_of(w):
    hi, lo = split(w)
    row = jnp.concatenate([hi, lo], axis=1)
    return jnp.concatenate([row, row], axis=0)


def mm(x, tile):
    hi, lo = split(x)
    both = jnp.concatenate([hi, lo], axis=1)
    out = jnp.dot(both, tile, preferred_element_type=F32)
    return out[:, :W] + out[:, W:]


def mm_pair(a, l, tile):
    ah, al = split(a)
    lh, ll = split(l)
    hi = jnp.concatenate([ah, lh], axis=1)
    lo = jnp.concatenate([al, ll], axis=1)
    out = jnp.dot(jnp.concatenate([hi, lo], axis=0), tile, preferred_element_type=F32)
    m = a.shape[0]
    out = out[:m] + out[m:]
    return out[:, :W] + out[:, W:]


def kernel(
    u_ref, l_ref, p_ref, g1_ref, g2_ref, s1_ref, s2_ref, out_ref,
    tu, tp, tl, tab, zs, v2, v1,
    g_c, g_z, g_y, t_c, t_z, t_y, h_c, h_z, h_y, r_c, r_z, ae, le,
    sg, halo, ss, ps, pr, lt,
    sem_c, sem_z, sem_y, sem_hc, sem_hz, sem_hy, sem_s, sem_own, sem_halo, sem_p,
):
    d = lax.axis_index("rows")
    x = lax.axis_index("rhs")
    y, z, c = d // 8, (d // 2) % 4, d % 2

    def in_c(j):
        return (y * 8 + z * 2 + (c + j) % 2, x)

    def in_z(j):
        return (y * 8 + ((z + j) % 4) * 2 + c, x)

    def in_y(j):
        return (((y + j) % 4) * 8 + z * 2 + c, x)

    def in_x(j):
        return (d, (x + j) % 4)

    after, before = ((d + 1) % 32, x), ((d + 31) % 32, x)

    barrier = pltpu.get_barrier_semaphore()
    peers = [in_c(1)] + [f(j) for f in (in_z, in_y, in_x) for j in (1, 2, 3)] + [after, before]
    for peer in peers:
        pl.semaphore_signal(barrier, inc=1, device_id=peer, device_id_type=MESH)

    own = [
        pltpu.make_async_copy(s, sg.at[x, t], sem_own.at[t]) for t, s in enumerate((s1_ref, s2_ref))
    ]
    for copy in own:
        copy.start()
    states = [
        pltpu.make_async_remote_copy(
            src_ref=sg.at[x], dst_ref=sg.at[x],
            send_sem=sem_s.at[0, j - 1], recv_sem=sem_s.at[1, j - 1],
            device_id=in_x(j), device_id_type=MESH,
        )
        for j in (1, 3, 2)
    ]

    def run(steps, step, carry, by=4):
        def some(b, carry):
            for s in range(by):
                carry = step(b * by + s, carry)
            return carry

        return lax.fori_loop(0, steps // by, some, carry)

    def spread(ref, me, size, where, sem):
        copies = [
            pltpu.make_async_remote_copy(
                src_ref=ref.at[me], dst_ref=ref.at[me],
                send_sem=sem.at[0, j - 1], recv_sem=sem.at[1, j - 1],
                device_id=where(j), device_id_type=MESH,
            )
            for j in range(1, size)
        ]
        for copy in copies:
            copy.start()
        return copies

    def finish(copies):
        for copy in copies:
            copy.wait()

    eye = (
        lax.broadcasted_iota(jnp.int32, (W, W), 0) == lax.broadcasted_iota(jnp.int32, (W, W), 1)
    ).astype(F32)
    zero_m = jnp.zeros((W, W), F32)
    zero_v = jnp.zeros((R, W), F32)

    def up_first(i, carry):
        tile = tile_of(u_ref[i])
        tu[i] = tile
        tile_p = tile_of(p_ref[i])
        tp[i] = tile_p
        yv = jnp.concatenate([g2_ref[i], zero_m], axis=0) - carry
        zs[i] = mm(yv, tile_p)
        return mm(yv, tile)

    carry = run(N, up_first, jnp.concatenate([zero_v, eye], axis=0))
    pl.semaphore_wait(barrier, len(peers))
    for copy in own:
        copy.wait()
    for copy in states:
        copy.start()
    g_c[c, EF:EH] = carry[:R]
    g_c[c, EM:EN] = carry[R:]

    def down_first(k, carry):
        i = N - 1 - k
        tile = tile_of(l_ref[i])
        tl[i] = tile
        vv = jnp.concatenate([zs[i], zero_m], axis=0) - carry
        v2[i] = vv[:R]
        hi, lo = split(vv[R:])
        tab[i] = jnp.concatenate([hi, lo], axis=1)
        return mm(vv, tile)

    carry = run(N, down_first, jnp.concatenate([zero_v, zero_m, eye], axis=0))
    g_c[c, EH:ES] = carry[:R]
    g_c[c, EN:EK] = carry[R : R + W]
    g_c[c, EK:EF] = carry[R + W :]

    half = pl.ds(pl.multiple_of(c * (ES // 2), 8), ES // 2)

    def gather_first(g, t, me, size, where, sem):
        if size == 2:
            finish(spread(g, me, size, where, sem))
        else:
            copies, passed = [], []
            for j in range(1, size):
                source = (me + size - j) % size
                copies.append(pltpu.make_async_remote_copy(
                    src_ref=g.at[me, half], dst_ref=g.at[me, half],
                    send_sem=sem.at[0, j - 1], recv_sem=sem.at[1, j - 1],
                    device_id=where(j), device_id_type=MESH,
                ))
                passed.append(pltpu.make_async_remote_copy(
                    src_ref=g.at[source, half], dst_ref=g.at[source, half],
                    send_sem=sem.at[2, j - 1], recv_sem=sem.at[3, j - 1],
                    device_id=in_c(1), device_id_type=MESH,
                ))
            for j in (1, 3, 2):
                copies[j - 1].start()
            for j in (1, 3, 2):
                copies[j - 1].wait_recv()
                passed[j - 1].start()
            for copy in copies:
                copy.wait_send()
            finish(passed)
        for e in range(size):
            for m in range(3):
                t[e, m] = tile_of(g[e, m * W : (m + 1) * W])

    def level_maps(g, t, r, me, size):
        a = jnp.concatenate([zero_v, eye], axis=0)
        many = []
        for e in range(size):
            ae[e] = a
            many.append(a)
            a = mm(a, t[e, 0]) + jnp.concatenate([g[e, EF:EH], zero_m], axis=0)
        l = jnp.concatenate([zero_v, zero_m, eye], axis=0)
        for e in reversed(range(size)):
            le[e] = l
            source = jnp.concatenate([g[e, EH:ES], zero_m], axis=0) + mm(many[e], t[e, 1])
            l = mm(l, t[e, 2]) + jnp.concatenate([source, zero_m], axis=0)
        r[0] = tile_of(ae[me, R:])
        r[1] = tile_of(le[me, R : R + W])
        r[2] = tile_of(le[me, R + W :])
        return (a, l), (ae[me, :R], le[me, :R])

    def level(vec, t, me, size):
        a = zero_v
        many = []
        for e in range(size):
            ae[e, :R] = a
            many.append(a)
            a = mm(a, t[e, 0]) + vec(e, 0)
        l = zero_v
        for e in reversed(range(size)):
            le[e, :R] = l
            l = mm(l, t[e, 2]) + (vec(e, 1) + mm(many[e], t[e, 1]))
        return (a, l), (ae[me, :R], le[me, :R])

    def put(g, me, a, l):
        g[me, EF:EH] = a[:R]
        g[me, EM:EN] = a[R:]
        g[me, EH:ES] = l[:R]
        g[me, EN:EK] = l[R : R + W]
        g[me, EK:EF] = l[R + W :]

    def enter(inside, r, a, l):
        return inside[0] + mm(a, r[0]), inside[1] + mm(a, r[1]) + mm(l, r[2])

    def vec_of(g):
        return lambda e, side: g[e, EF + R * side : EF + R * side + R]

    def vec_small(h):
        return lambda e, side: h[e, R * side : R * side + R]

    gather_first(g_c, t_c, c, 2, in_c, sem_c)
    total, inside_c = level_maps(g_c, t_c, r_c, c, 2)
    put(g_z, z, *total)
    gather_first(g_z, t_z, z, 4, in_z, sem_z)
    total, inside_z = level_maps(g_z, t_z, r_z, z, 4)
    put(g_y, y, *total)
    gather_first(g_y, t_y, y, 4, in_y, sem_y)
    _, (a, l) = level(vec_of(g_y), t_y, y, 4)
    a, l = enter(inside_z, r_z, a, l)
    a, l = enter(inside_c, r_c, a, l)

    def settle(v, a, l):
        for i in range(N):
            v[i] = v[i] + mm_pair(a, l, tab[i])

    settle(v2, a, l)

    block_of = lax.broadcasted_iota(jnp.int32, (W, W), 1) // R

    def share(v, t):
        groups = [v[4 * q : 4 * q + 4].reshape(W, W) for q in range(4)]
        for dest in range(4):
            piece = groups[dest]
            for q in range(4):
                if q != dest:
                    moved = pltpu.roll(groups[q], (R * (q - dest)) % W, 1)
                    piece = jnp.where(block_of == q, moved, piece)
            if True:
                own_q = groups[dest]
                piece = jnp.where(block_of == dest, own_q, piece)
            ps[t, dest] = piece
        pr[t, x] = ps[t, x]
        copies = [
            pltpu.make_async_remote_copy(
                src_ref=ps.at[t, (x + j) % 4], dst_ref=pr.at[t, x],
                send_sem=sem_p.at[t, 0, j - 1], recv_sem=sem_p.at[t, 1, j - 1],
                device_id=in_x(j), device_id_type=MESH,
            )
            for j in (1, 3, 2)
        ]
        for copy in copies:
            copy.start()
        return copies

    shared_two = share(v2, 1)

    def up(i, carry):
        yv = g1_ref[i] + v2[i] - carry
        zs[i, :R] = mm(yv, tp[i])
        return mm(yv, tu[i])

    h_c[c, :R] = run(N, up, zero_v)

    def down(k, carry):
        i = N - 1 - k
        vv = zs[i, :R] - carry
        v1[i] = vv
        return mm(vv, tl[i])

    h_c[c, R:] = run(N, down, zero_v)

    finish(spread(h_c, c, 2, in_c, sem_hc))
    (a, l), inside_c = level(vec_small(h_c), t_c, c, 2)
    h_z[z, :R] = a
    h_z[z, R:] = l
    in_flight = spread(h_z, z, 4, in_z, sem_hz)

    finish(states)
    edges = []
    for side, (row, where) in enumerate(((N - 1, after), (0, before))):
        for q in range(4):
            copy = pltpu.make_async_remote_copy(
                src_ref=sg.at[q, :, row], dst_ref=halo.at[side, q],
                send_sem=sem_halo.at[0, side, q], recv_sem=sem_halo.at[1, side, q],
                device_id=where, device_id_type=MESH,
            )
            copy.start()
            edges.append(copy)

    def operand(parts):
        hi, lo = split(jnp.concatenate(parts, axis=0))
        return jnp.concatenate([hi, lo], axis=1)

    def pack(i, none):
        ss[i + 1] = operand([sg[q, t, i] for t in range(2) for q in range(4)])
        return none

    run(N, pack, 0)

    finish(in_flight)
    (a, l), inside_z = level(vec_small(h_z), t_z, z, 4)
    h_y[y, :R] = a
    h_y[y, R:] = l
    in_flight = spread(h_y, y, 4, in_y, sem_hy)

    finish(edges)
    keep = ((d > 0).astype(F32), (d < 31).astype(F32))
    for side, slot in ((0, 0), (1, N + 1)):
        ss[slot] = operand([halo[side, q, t] * keep[side] for t in range(2) for q in range(4)])

    finish(in_flight)
    _, (a, l) = level(vec_small(h_y), t_y, y, 4)
    a, l = enter(inside_z, r_z, a, l)
    a, l = enter(inside_c, r_c, a, l)
    settle(v1, a, l)
    finish(shared_two)
    shared_one = share(v1, 0)

    def turn(t):
        for sub in range(4):
            stack = jnp.concatenate(
                [pr[t, q, R * sub : R * sub + R] for q in range(4)], axis=0
            ).T
            hi, lo = split(stack)
            for q in range(4):
                lt[4 * q + sub, :R, t * W : (t + 1) * W] = hi[R * q : R * q + R]
                lt[4 * q + sub, R:, t * W : (t + 1) * W] = lo[R * q : R * q + R]

    turn(1)
    finish(shared_one)
    turn(0)

    def grads(i, none):
        for k, j in enumerate((1, 0, 2)):
            o = jnp.dot(lt[i], ss[i + j], preferred_element_type=F32)
            o = o[:R] + o[R:]
            out_ref[k, i] = -(o[:, :W] + o[:, W:])
        return none

    run(N, grads, 0)


def body(upper_unit, lower_unit, pivot_inv, loss_grad_one, loss_grad_two, state_one, state_two):
    vmem = pl.BlockSpec(memory_space=pltpu.VMEM)
    anywhere = pl.BlockSpec(memory_space=pl.ANY)
    dma = pltpu.SemaphoreType.DMA
    tile = (2 * W, 2 * W)
    grads = pl.pallas_call(
        kernel,
        out_shape=jax.ShapeDtypeStruct((3, N, R, W), F32),
        in_specs=[vmem] * 5 + [anywhere] * 2,
        out_specs=vmem,
        scratch_shapes=[
            pltpu.VMEM((N, *tile), BF16),
            pltpu.VMEM((N, *tile), BF16),
            pltpu.VMEM((N, *tile), BF16),
            pltpu.VMEM((N, *tile), BF16),
            pltpu.VMEM((N, R + W, W), F32),
            pltpu.VMEM((N, R, W), F32),
            pltpu.VMEM((N, R, W), F32),
            pltpu.VMEM((2, ES, W), F32),
            pltpu.VMEM((4, ES, W), F32),
            pltpu.VMEM((4, ES, W), F32),
            pltpu.VMEM((2, 3, *tile), BF16),
            pltpu.VMEM((4, 3, *tile), BF16),
            pltpu.VMEM((4, 3, *tile), BF16),
            pltpu.VMEM((2, 2 * R, W), F32),
            pltpu.VMEM((4, 2 * R, W), F32),
            pltpu.VMEM((4, 2 * R, W), F32),
            pltpu.VMEM((3, *tile), BF16),
            pltpu.VMEM((3, *tile), BF16),
            pltpu.VMEM((4, R + W, W), F32),
            pltpu.VMEM((4, R + 2 * W, W), F32),
            pltpu.VMEM((4, 2, N, R, W), F32),
            pltpu.VMEM((2, 4, 2, R, W), F32),
            pltpu.VMEM((N + 2, *tile), BF16),
            pltpu.VMEM((2, 4, W, W), F32),
            pltpu.VMEM((2, 4, W, W), F32),
            pltpu.VMEM((N, 2 * R, 2 * W), BF16),
            dma((2, 1)), dma((4, 3)), dma((4, 3)),
            dma((2, 1)), dma((2, 3)), dma((2, 3)),
            dma((2, 3)), dma((2,)), dma((2, 2, 4)), dma((2, 2, 3)),
        ],
        compiler_params=pltpu.CompilerParams(
            collective_id=0, has_side_effects=True, vmem_limit_bytes=60 * 2**20
        ),
    )(upper_unit, lower_unit, pivot_inv, loss_grad_one, loss_grad_two, state_one, state_two)
    return jnp.transpose(grads, (2, 0, 1, 3))


def solution(mesh):
    by_rows = P("rows", None, None)
    by_both = P("rows", "rhs", None)
    return jax.shard_map(
        body,
        mesh=mesh,
        in_specs=(by_rows,) * 3 + (by_both,) * 4,
        out_specs=P("rhs", None, "rows", None),
        check_vma=False,
    )
```

```python
import jax
import jax.numpy as jnp
from jax import lax
from jax.experimental import pallas as pl
from jax.experimental.pallas import tpu as pltpu
from jax.sharding import PartitionSpec as P

MESH = pl.DeviceIdType.MESH
F32, BF16 = jnp.float32, jnp.bfloat16
N = 16
W = 128
R = 32
EM, EK, EF, EN, EH, ES = 0, 128, 256, 288, 416, 448
PARTS = ((0, EN), (EN, ES - EN))


def split(x):
    hi = x.astype(BF16)
    lo = (x - hi.astype(F32)).astype(BF16)
    return hi, lo


def tile_of(w):
    hi, lo = split(w)
    row = jnp.concatenate([hi, lo], axis=1)
    return jnp.concatenate([row, row], axis=0)


def mm(x, tile):
    hi, lo = split(x)
    both = jnp.concatenate([hi, lo], axis=1)
    out = jnp.dot(both, tile, preferred_element_type=F32)
    return out[:, :W] + out[:, W:]


def mm_pair(a, l, tile):
    ah, al = split(a)
    lh, ll = split(l)
    hi = jnp.concatenate([ah, lh], axis=1)
    lo = jnp.concatenate([al, ll], axis=1)
    out = jnp.dot(jnp.concatenate([hi, lo], axis=0), tile, preferred_element_type=F32)
    m = a.shape[0]
    out = out[:m] + out[m:]
    return out[:, :W] + out[:, W:]


def kernel(
    u_in, l_in, p_in, g1_in, g2_in, s1_ref, s2_ref, out_ref,
    u_ref, l_ref, p_ref, g1_ref, g2_ref,
    tu, tp, tl, tab, zs, v2, v1,
    g_c, g_z, g_y, t_c, t_z, t_y, h_c, h_z, h_y, r_c, r_z, ae_c, ae_z, ke, ae, le,
    sg, halo, ss, ps, pr, lt,
    sem_c, sem_z, sem_y, sem_hc, sem_hz, sem_hy, sem_s, sem_own, sem_halo, sem_p, sem_in,
):
    d = lax.axis_index("rows")
    x = lax.axis_index("rhs")
    y, z, c = d // 8, (d // 2) % 4, d % 2

    def in_c(j):
        return (y * 8 + z * 2 + (c + j) % 2, x)

    def in_z(j):
        return (y * 8 + ((z + j) % 4) * 2 + c, x)

    def in_y(j):
        return (((y + j) % 4) * 8 + z * 2 + c, x)

    def in_x(j):
        return (d, (x + j) % 4)

    after, before = ((d + 1) % 32, x), ((d + 31) % 32, x)

    barrier = pltpu.get_barrier_semaphore()
    peers = [in_c(1)] + [f(j) for f in (in_z, in_y, in_x) for j in (1, 2, 3)] + [after, before]
    for peer in peers:
        pl.semaphore_signal(barrier, inc=1, device_id=peer, device_id_type=MESH)

    loads = [
        pltpu.make_async_copy(src, dst, sem_in.at[k])
        for k, (src, dst) in enumerate((
            (u_in, u_ref), (l_in, l_ref), (g2_in, g2_ref), (p_in, p_ref), (g1_in, g1_ref)
        ))
    ]
    for copy in loads:
        copy.start()
    own = [
        pltpu.make_async_copy(s, sg.at[x, t], sem_own.at[t]) for t, s in enumerate((s1_ref, s2_ref))
    ]
    for copy in own:
        copy.start()
    states = [
        pltpu.make_async_remote_copy(
            src_ref=sg.at[x], dst_ref=sg.at[x],
            send_sem=sem_s.at[0, j - 1], recv_sem=sem_s.at[1, j - 1],
            device_id=in_x(j), device_id_type=MESH,
        )
        for j in (1, 3, 2)
    ]

    def run(steps, step, carry, by=4):
        def some(b, carry):
            for s in range(by):
                carry = step(b * by + s, carry)
            return carry

        return lax.fori_loop(0, steps // by, some, carry)

    def spread(ref, me, size, where, sem):
        copies = [
            pltpu.make_async_remote_copy(
                src_ref=ref.at[me], dst_ref=ref.at[me],
                send_sem=sem.at[0, j - 1], recv_sem=sem.at[1, j - 1],
                device_id=where(j), device_id_type=MESH,
            )
            for j in range(1, size)
        ]
        for copy in copies:
            copy.start()
        return copies

    def finish(copies):
        for copy in copies:
            copy.wait()

    eye = (
        lax.broadcasted_iota(jnp.int32, (W, W), 0) == lax.broadcasted_iota(jnp.int32, (W, W), 1)
    ).astype(F32)
    zero_m = jnp.zeros((W, W), F32)
    zero_v = jnp.zeros((R, W), F32)

    def first(i, carry):
        right, left = carry
        tile, tile_p = tile_of(u_ref[i]), tile_of(p_ref[i])
        tu[i] = tile
        tp[i] = tile_p
        yv = jnp.concatenate([g2_ref[i], zero_m], axis=0) - right
        zs[i] = mm(yv, tile_p)
        k = N - 1 - i
        tile_l = tile_of(l_ref[k])
        tl[k] = tile_l
        vv = -left
        hi, lo = split(vv)
        tab[k, W:] = jnp.concatenate([hi, lo], axis=1)
        return mm(yv, tile), mm(vv, tile_l)

    for copy in loads:
        copy.wait()
    right, left = run(N, first, (jnp.concatenate([zero_v, eye], axis=0), eye))
    g_c[c, EF:EN] = right[:R]
    g_c[c, EM:EK] = right[R:]
    g_c[c, EK:EF] = left

    pl.semaphore_wait(barrier, len(peers))

    def pair(part):
        rows = pl.ds(*PARTS[part])
        copy = pltpu.make_async_remote_copy(
            src_ref=g_c.at[c, rows], dst_ref=g_c.at[c, rows],
            send_sem=sem_c.at[part, 0], recv_sem=sem_c.at[part, 1],
            device_id=in_c(1), device_id_type=MESH,
        )
        copy.start()
        return copy

    def send_part(g, part, me, where, sem):
        low, size = PARTS[part]
        rows = pl.ds(pl.multiple_of(low + c * (size // 2), 8), size // 2)
        copies, passed = [], []
        for j in range(1, 4):
            source = (me + 4 - j) % 4
            copies.append(pltpu.make_async_remote_copy(
                src_ref=g.at[me, rows], dst_ref=g.at[me, rows],
                send_sem=sem.at[part, 0, j - 1], recv_sem=sem.at[part, 1, j - 1],
                device_id=where(j), device_id_type=MESH,
            ))
            passed.append(pltpu.make_async_remote_copy(
                src_ref=g.at[source, rows], dst_ref=g.at[source, rows],
                send_sem=sem.at[part, 2, j - 1], recv_sem=sem.at[part, 3, j - 1],
                device_id=in_c(1), device_id_type=MESH,
            ))
        for j in (1, 3, 2):
            copies[j - 1].start()
        return copies, passed

    def pass_on(flight):
        copies, passed = flight
        for j in (1, 3, 2):
            copies[j - 1].wait_recv()
            passed[j - 1].start()

    def land(flight):
        copies, passed = flight
        for copy in copies:
            copy.wait_send()
        for copy in passed:
            copy.wait()

    def tiles_mk(g, t, size):
        for e in range(size):
            t[e, 0] = tile_of(g[e, EM:EK])
            t[e, 2] = tile_of(g[e, EK:EF])

    def tiles_n(g, t, size):
        for e in range(size):
            t[e, 1] = tile_of(g[e, EN:EH])

    def level_mk(g, t, r, kept, me, size):
        a = jnp.concatenate([zero_v, eye], axis=0)
        k = eye
        for e in range(size):
            kept[e] = a
            a = mm(a, t[e, 0]) + jnp.concatenate([g[e, EF:EN], zero_m], axis=0)
            ke[size - 1 - e] = k
            k = mm(k, t[size - 1 - e, 2])
        r[0] = tile_of(kept[me, R:])
        r[2] = tile_of(ke[me])
        return a, k, kept[me, :R]

    def level_n(g, t, r, kept, me, size):
        l = jnp.concatenate([zero_v, zero_m], axis=0)
        for e in reversed(range(size)):
            le[e] = l
            l = (
                mm(l, t[e, 2])
                + jnp.concatenate([g[e, EH:ES], zero_m], axis=0)
                + mm(kept[e], t[e, 1])
            )
        r[1] = tile_of(le[me, R:])
        return l, le[me, :R]

    def put_mk(g, me, a, k):
        g[me, EF:EN] = a[:R]
        g[me, EM:EK] = a[R:]
        g[me, EK:EF] = k

    def put_n(g, me, l):
        g[me, EH:ES] = l[:R]
        g[me, EN:EH] = l[R:]

    def second(k, carry):
        i = N - 1 - k
        vv = zs[i] - carry
        v2[i] = vv[:R]
        hi, lo = split(vv[R:])
        tab[i, :W] = jnp.concatenate([hi, lo], axis=1)
        return mm(vv, tl[i])

    c1 = pair(0)
    for copy in own:
        copy.wait()
    for copy in states:
        copy.start()
    carry = run(N // 2, second, jnp.concatenate([zero_v, zero_m], axis=0))
    c1.wait()
    tiles_mk(g_c, t_c, 2)
    a_tot, k_tot, a_c = level_mk(g_c, t_c, r_c, ae_c, c, 2)
    put_mk(g_z, z, a_tot, k_tot)
    z1 = send_part(g_z, 0, z, in_z, sem_z)
    carry = run(N // 2, lambda k, v: second(k + N // 2, v), carry)
    put_n(g_c, c, carry)
    c2 = pair(1)
    c2.wait()
    tiles_n(g_c, t_c, 2)
    l_tot, l_c = level_n(g_c, t_c, r_c, ae_c, c, 2)
    put_n(g_z, z, l_tot)
    z2 = send_part(g_z, 1, z, in_z, sem_z)
    pass_on(z1)
    land(z1)
    tiles_mk(g_z, t_z, 4)
    a_tot, k_tot, a_z = level_mk(g_z, t_z, r_z, ae_z, z, 4)
    put_mk(g_y, y, a_tot, k_tot)
    y1 = send_part(g_y, 0, y, in_y, sem_y)
    pass_on(z2)
    land(z2)
    tiles_n(g_z, t_z, 4)
    l_tot, l_z = level_n(g_z, t_z, r_z, ae_z, z, 4)
    put_n(g_y, y, l_tot)
    y2 = send_part(g_y, 1, y, in_y, sem_y)
    pass_on(y1)
    land(y1)
    tiles_mk(g_y, t_y, 4)
    pass_on(y2)
    land(y2)
    tiles_n(g_y, t_y, 4)

    def level(vec, t, me, size):
        a = zero_v
        many = []
        for e in range(size):
            ae[e, :R] = a
            many.append(a)
            a = mm(a, t[e, 0]) + vec(e, 0)
        l = zero_v
        for e in reversed(range(size)):
            le[e, :R] = l
            l = mm(l, t[e, 2]) + (vec(e, 1) + mm(many[e], t[e, 1]))
        return (a, l), (ae[me, :R], le[me, :R])

    def enter(inside, r, a, l):
        return inside[0] + mm(a, r[0]), inside[1] + mm(a, r[1]) + mm(l, r[2])

    def vec_of(g):
        return lambda e, side: g[e, EH:ES] if side else g[e, EF:EN]

    def vec_small(h):
        return lambda e, side: h[e, R * side : R * side + R]

    _, (a, l) = level(vec_of(g_y), t_y, y, 4)
    a, l = enter((a_z, l_z), r_z, a, l)
    a, l = enter((a_c, l_c), r_c, a, l)

    def settle(v, a, l):
        for i in range(N):
            v[i] = v[i] + mm_pair(a, l, tab[i])

    settle(v2, a, l)

    block_of = lax.broadcasted_iota(jnp.int32, (W, W), 1) // R

    def share(v, t):
        groups = [v[4 * q : 4 * q + 4].reshape(W, W) for q in range(4)]
        for dest in range(4):
            piece = groups[dest]
            for q in range(4):
                if q != dest:
                    moved = pltpu.roll(groups[q], (R * (q - dest)) % W, 1)
                    piece = jnp.where(block_of == q, moved, piece)
            if True:
                own_q = groups[dest]
                piece = jnp.where(block_of == dest, own_q, piece)
            ps[t, dest] = piece
        pr[t, x] = ps[t, x]
        copies = [
            pltpu.make_async_remote_copy(
                src_ref=ps.at[t, (x + j) % 4], dst_ref=pr.at[t, x],
                send_sem=sem_p.at[t, 0, j - 1], recv_sem=sem_p.at[t, 1, j - 1],
                device_id=in_x(j), device_id_type=MESH,
            )
            for j in (1, 3, 2)
        ]
        for copy in copies:
            copy.start()
        return copies

    shared_two = share(v2, 1)

    def up(i, carry):
        yv = g1_ref[i] + v2[i] - carry
        zs[i, :R] = mm(yv, tp[i])
        return mm(yv, tu[i])

    h_c[c, :R] = run(N, up, zero_v)

    def down(k, carry):
        i = N - 1 - k
        vv = zs[i, :R] - carry
        v1[i] = vv
        return mm(vv, tl[i])

    h_c[c, R:] = run(N, down, zero_v)

    finish(spread(h_c, c, 2, in_c, sem_hc))
    (a, l), inside_c = level(vec_small(h_c), t_c, c, 2)
    h_z[z, :R] = a
    h_z[z, R:] = l
    in_flight = spread(h_z, z, 4, in_z, sem_hz)

    finish(states)
    edges = []
    for side, (row, where) in enumerate(((N - 1, after), (0, before))):
        for q in range(4):
            copy = pltpu.make_async_remote_copy(
                src_ref=sg.at[q, :, row], dst_ref=halo.at[side, q],
                send_sem=sem_halo.at[0, side, q], recv_sem=sem_halo.at[1, side, q],
                device_id=where, device_id_type=MESH,
            )
            copy.start()
            edges.append(copy)

    def operand(parts):
        hi, lo = split(jnp.concatenate(parts, axis=0))
        return jnp.concatenate([hi, lo], axis=1)

    def pack(i, none):
        ss[i + 1] = operand([sg[q, t, i] for t in range(2) for q in range(4)])
        return none

    run(N, pack, 0)

    finish(in_flight)
    (a, l), inside_z = level(vec_small(h_z), t_z, z, 4)
    h_y[y, :R] = a
    h_y[y, R:] = l
    in_flight = spread(h_y, y, 4, in_y, sem_hy)

    finish(edges)
    keep = ((d > 0).astype(F32), (d < 31).astype(F32))
    for side, slot in ((0, 0), (1, N + 1)):
        ss[slot] = operand([halo[side, q, t] * keep[side] for t in range(2) for q in range(4)])

    finish(in_flight)
    _, (a, l) = level(vec_small(h_y), t_y, y, 4)
    a, l = enter(inside_z, r_z, a, l)
    a, l = enter(inside_c, r_c, a, l)
    settle(v1, a, l)
    finish(shared_two)
    shared_one = share(v1, 0)

    def turn(t):
        for sub in range(4):
            stack = jnp.concatenate(
                [pr[t, q, R * sub : R * sub + R] for q in range(4)], axis=0
            ).T
            hi, lo = split(stack)
            for q in range(4):
                lt[4 * q + sub, :R, t * W : (t + 1) * W] = hi[R * q : R * q + R]
                lt[4 * q + sub, R:, t * W : (t + 1) * W] = lo[R * q : R * q + R]

    turn(1)
    finish(shared_one)
    turn(0)

    def grads(i, none):
        for k, j in enumerate((1, 0, 2)):
            o = jnp.dot(lt[i], ss[i + j], preferred_element_type=F32)
            o = o[:R] + o[R:]
            out_ref[k, i] = -(o[:, :W] + o[:, W:])
        return none

    run(N, grads, 0)


def body(upper_unit, lower_unit, pivot_inv, loss_grad_one, loss_grad_two, state_one, state_two):
    vmem = pl.BlockSpec(memory_space=pltpu.VMEM)
    anywhere = pl.BlockSpec(memory_space=pl.ANY)
    dma = pltpu.SemaphoreType.DMA
    tile = (2 * W, 2 * W)
    grads = pl.pallas_call(
        kernel,
        out_shape=jax.ShapeDtypeStruct((3, N, R, W), F32),
        in_specs=[anywhere] * 7,
        out_specs=vmem,
        scratch_shapes=[
            pltpu.VMEM((N, W, W), F32),
            pltpu.VMEM((N, W, W), F32),
            pltpu.VMEM((N, W, W), F32),
            pltpu.VMEM((N, R, W), F32),
            pltpu.VMEM((N, R, W), F32),
            pltpu.VMEM((N, *tile), BF16),
            pltpu.VMEM((N, *tile), BF16),
            pltpu.VMEM((N, *tile), BF16),
            pltpu.VMEM((N, *tile), BF16),
            pltpu.VMEM((N, R + W, W), F32),
            pltpu.VMEM((N, R, W), F32),
            pltpu.VMEM((N, R, W), F32),
            pltpu.VMEM((2, ES, W), F32),
            pltpu.VMEM((4, ES, W), F32),
            pltpu.VMEM((4, ES, W), F32),
            pltpu.VMEM((2, 3, *tile), BF16),
            pltpu.VMEM((4, 3, *tile), BF16),
            pltpu.VMEM((4, 3, *tile), BF16),
            pltpu.VMEM((2, 2 * R, W), F32),
            pltpu.VMEM((4, 2 * R, W), F32),
            pltpu.VMEM((4, 2 * R, W), F32),
            pltpu.VMEM((3, *tile), BF16),
            pltpu.VMEM((3, *tile), BF16),
            pltpu.VMEM((2, R + W, W), F32),
            pltpu.VMEM((4, R + W, W), F32),
            pltpu.VMEM((4, W, W), F32),
            pltpu.VMEM((4, R, W), F32),
            pltpu.VMEM((4, R + W, W), F32),
            pltpu.VMEM((4, 2, N, R, W), F32),
            pltpu.VMEM((2, 4, 2, R, W), F32),
            pltpu.VMEM((N + 2, *tile), BF16),
            pltpu.VMEM((2, 4, W, W), F32),
            pltpu.VMEM((2, 4, W, W), F32),
            pltpu.VMEM((N, 2 * R, 2 * W), BF16),
            dma((2, 2)), dma((2, 4, 3)), dma((2, 4, 3)),
            dma((2, 1)), dma((2, 3)), dma((2, 3)),
            dma((2, 3)), dma((2,)), dma((2, 2, 4)), dma((2, 2, 3)), dma((5,)),
        ],
        compiler_params=pltpu.CompilerParams(
            collective_id=0, has_side_effects=True, vmem_limit_bytes=60 * 2**20
        ),
    )(upper_unit, lower_unit, pivot_inv, loss_grad_one, loss_grad_two, state_one, state_two)
    return jnp.transpose(grads, (2, 0, 1, 3))


def solution(mesh):
    by_rows = P("rows", None, None)
    by_both = P("rows", "rhs", None)
    return jax.shard_map(
        body,
        mesh=mesh,
        in_specs=(by_rows,) * 3 + (by_both,) * 4,
        out_specs=P("rhs", None, "rows", None),
        check_vma=False,
    )
```

```python
import jax
import jax.numpy as jnp
from jax import lax
from jax.experimental import pallas as pl
from jax.experimental.pallas import tpu as pltpu
from jax.sharding import PartitionSpec as P

MESH = pl.DeviceIdType.MESH
F32, BF16 = jnp.float32, jnp.bfloat16
N = 16
W = 128
R = 32
EM, EK, EF, EN, EH, ES = 0, 128, 256, 288, 416, 448
PARTS = ((0, EN), (EN, ES - EN))


def split(x):
    hi = x.astype(BF16)
    lo = (x - hi.astype(F32)).astype(BF16)
    return hi, lo


def tile_of(w):
    hi, lo = split(w)
    row = jnp.concatenate([hi, lo], axis=1)
    return jnp.concatenate([row, row], axis=0)


def mm(x, tile):
    hi, lo = split(x)
    both = jnp.concatenate([hi, lo], axis=1)
    out = jnp.dot(both, tile, preferred_element_type=F32)
    return out[:, :W] + out[:, W:]


def mm_pair(a, l, tile):
    ah, al = split(a)
    lh, ll = split(l)
    hi = jnp.concatenate([ah, lh], axis=1)
    lo = jnp.concatenate([al, ll], axis=1)
    out = jnp.dot(jnp.concatenate([hi, lo], axis=0), tile, preferred_element_type=F32)
    m = a.shape[0]
    out = out[:m] + out[m:]
    return out[:, :W] + out[:, W:]


def kernel(
    u_in, l_in, p_in, g1_in, g2_in, s1_ref, s2_ref, out_ref,
    u_ref, l_ref, p_ref, g1_ref, g2_ref,
    tu, tp, tl, tab, tab1, zs, zs3, v2, v1, base, sl, fh, tfh, al,
    g_c, g_z, g_y, t_c, t_z, t_y, h_c, h_z, h_y, r_c, r_z, ae_c, ae_z, ke, ae, le,
    sg, halo, ss, ps, pr, lt,
    sem_c, sem_z, sem_y, sem_hc, sem_hz, sem_hy, sem_s, sem_own, sem_halo, sem_p, sem_in, sem_al,
):
    d = lax.axis_index("rows")
    x = lax.axis_index("rhs")
    y, z, c = d // 8, (d // 2) % 4, d % 2

    def in_c(j):
        return (y * 8 + z * 2 + (c + j) % 2, x)

    def in_z(j):
        return (y * 8 + ((z + j) % 4) * 2 + c, x)

    def in_y(j):
        return (((y + j) % 4) * 8 + z * 2 + c, x)

    def in_x(j):
        return (d, (x + j) % 4)

    after, before = ((d + 1) % 32, x), ((d + 31) % 32, x)

    barrier = pltpu.get_barrier_semaphore()
    peers = [in_c(1)] + [f(j) for f in (in_z, in_y, in_x) for j in (1, 2, 3)] + [after, before]
    for peer in peers:
        pl.semaphore_signal(barrier, inc=1, device_id=peer, device_id_type=MESH)

    loads = [
        pltpu.make_async_copy(src, dst, sem_in.at[k])
        for k, (src, dst) in enumerate((
            (u_in, u_ref), (l_in, l_ref), (g2_in, g2_ref), (p_in, p_ref), (g1_in, g1_ref)
        ))
    ]
    for copy in loads:
        copy.start()
    own = [
        pltpu.make_async_copy(s, sg.at[x, t], sem_own.at[t]) for t, s in enumerate((s1_ref, s2_ref))
    ]
    for copy in own:
        copy.start()
    states = [
        pltpu.make_async_remote_copy(
            src_ref=sg.at[x], dst_ref=sg.at[x],
            send_sem=sem_s.at[0, j - 1], recv_sem=sem_s.at[1, j - 1],
            device_id=in_x(j), device_id_type=MESH,
        )
        for j in (1, 3, 2)
    ]

    def run(steps, step, carry, by=4):
        def some(b, carry):
            for s in range(by):
                carry = step(b * by + s, carry)
            return carry

        return lax.fori_loop(0, steps // by, some, carry)

    def spread(ref, me, size, where, sem):
        copies = [
            pltpu.make_async_remote_copy(
                src_ref=ref.at[me], dst_ref=ref.at[me],
                send_sem=sem.at[0, j - 1], recv_sem=sem.at[1, j - 1],
                device_id=where(j), device_id_type=MESH,
            )
            for j in range(1, size)
        ]
        for copy in copies:
            copy.start()
        return copies

    def finish(copies):
        for copy in copies:
            copy.wait()

    eye = (
        lax.broadcasted_iota(jnp.int32, (W, W), 0) == lax.broadcasted_iota(jnp.int32, (W, W), 1)
    ).astype(F32)
    zero_m = jnp.zeros((W, W), F32)
    zero_v = jnp.zeros((R, W), F32)

    def first(i, carry):
        right, left = carry
        tile, tile_p = tile_of(u_ref[i]), tile_of(p_ref[i])
        tu[i] = tile
        tp[i] = tile_p
        yv = jnp.concatenate([g2_ref[i], zero_m], axis=0) - right
        zs[i] = mm(yv, tile_p)
        k = N - 1 - i
        tile_l = tile_of(l_ref[k])
        tl[k] = tile_l
        vv = -left
        hi, lo = split(vv)
        tab[k, W:] = jnp.concatenate([hi, lo], axis=1)
        return mm(yv, tile), mm(vv, tile_l)

    for copy in loads:
        copy.wait()
    right, left = run(N, first, (jnp.concatenate([zero_v, eye], axis=0), eye))
    g_c[c, EF:EN] = right[:R]
    g_c[c, EM:EK] = right[R:]
    g_c[c, EK:EF] = left

    pl.semaphore_wait(barrier, len(peers))

    def pair(part):
        rows = pl.ds(*PARTS[part])
        copy = pltpu.make_async_remote_copy(
            src_ref=g_c.at[c, rows], dst_ref=g_c.at[c, rows],
            send_sem=sem_c.at[part, 0], recv_sem=sem_c.at[part, 1],
            device_id=in_c(1), device_id_type=MESH,
        )
        copy.start()
        return copy

    def send_part(g, part, me, where, sem):
        low, size = PARTS[part]
        rows = pl.ds(pl.multiple_of(low + c * (size // 2), 8), size // 2)
        copies, passed = [], []
        for j in range(1, 4):
            source = (me + 4 - j) % 4
            copies.append(pltpu.make_async_remote_copy(
                src_ref=g.at[me, rows], dst_ref=g.at[me, rows],
                send_sem=sem.at[part, 0, j - 1], recv_sem=sem.at[part, 1, j - 1],
                device_id=where(j), device_id_type=MESH,
            ))
            passed.append(pltpu.make_async_remote_copy(
                src_ref=g.at[source, rows], dst_ref=g.at[source, rows],
                send_sem=sem.at[part, 2, j - 1], recv_sem=sem.at[part, 3, j - 1],
                device_id=in_c(1), device_id_type=MESH,
            ))
        for j in (1, 3, 2):
            copies[j - 1].start()
        return copies, passed

    def pass_on(flight):
        copies, passed = flight
        for j in (1, 3, 2):
            copies[j - 1].wait_recv()
            passed[j - 1].start()

    def land(flight):
        copies, passed = flight
        for copy in copies:
            copy.wait_send()
        for copy in passed:
            copy.wait()

    def tiles_mk(g, t, size):
        for e in range(size):
            t[e, 0] = tile_of(g[e, EM:EK])
            t[e, 2] = tile_of(g[e, EK:EF])

    def tiles_n(g, t, size):
        for e in range(size):
            t[e, 1] = tile_of(g[e, EN:EH])

    def level_mk(g, t, r, kept, me, size):
        a = jnp.concatenate([zero_v, eye], axis=0)
        k = eye
        for e in range(size):
            kept[e] = a
            a = mm(a, t[e, 0]) + jnp.concatenate([g[e, EF:EN], zero_m], axis=0)
            ke[size - 1 - e] = k
            k = mm(k, t[size - 1 - e, 2])
        r[0] = tile_of(kept[me, R:])
        r[2] = tile_of(ke[me])
        return a, k, kept[me, :R]

    def level_n(g, t, r, kept, me, size):
        l = jnp.concatenate([zero_v, zero_m], axis=0)
        for e in reversed(range(size)):
            le[e] = l
            l = (
                mm(l, t[e, 2])
                + jnp.concatenate([g[e, EH:ES], zero_m], axis=0)
                + mm(kept[e], t[e, 1])
            )
        r[1] = tile_of(le[me, R:])
        return l, le[me, :R]

    def put_mk(g, me, a, k):
        g[me, EF:EN] = a[:R]
        g[me, EM:EK] = a[R:]
        g[me, EK:EF] = k

    def put_n(g, me, l):
        g[me, EH:ES] = l[:R]
        g[me, EN:EH] = l[R:]

    def second(k, carry):
        i = N - 1 - k
        vv = zs[i] - carry
        v2[i] = vv[:R]
        hi, lo = split(vv[R:])
        tab[i, :W] = jnp.concatenate([hi, lo], axis=1)
        return mm(vv, tl[i])

    c1 = pair(0)
    for copy in own:
        copy.wait()
    for copy in states:
        copy.start()
    carry = run(N // 2, second, jnp.concatenate([zero_v, zero_m], axis=0))
    c1.wait()
    tiles_mk(g_c, t_c, 2)
    a_tot, k_tot, a_c = level_mk(g_c, t_c, r_c, ae_c, c, 2)
    put_mk(g_z, z, a_tot, k_tot)
    z1 = send_part(g_z, 0, z, in_z, sem_z)
    carry = run(N // 2, lambda k, v: second(k + N // 2, v), carry)
    put_n(g_c, c, carry)
    c2 = pair(1)
    c2.wait()
    tiles_n(g_c, t_c, 2)
    l_tot, l_c = level_n(g_c, t_c, r_c, ae_c, c, 2)
    put_n(g_z, z, l_tot)
    z2 = send_part(g_z, 1, z, in_z, sem_z)

    def third(i, carry):
        responses = tab[i, :, :W].astype(F32) + tab[i, :, W:].astype(F32)
        yv = jnp.concatenate([g1_ref[i] + v2[i], responses], axis=0) - carry
        zs3[i] = mm(yv, tp[i])
        return mm(yv, tu[i])

    def fourth(k, carry):
        i = N - 1 - k
        vv = zs3[i] - carry
        v1[i] = vv[:R]
        hi, lo = split(vv[R:])
        tab1[i] = jnp.concatenate([hi, lo], axis=1)
        return mm(vv, tl[i])

    def keep_ends(side, carry):
        fh[side] = carry[:R]
        hi, lo = split(carry[R:])
        tfh[side] = jnp.concatenate([hi, lo], axis=1)

    nothing = jnp.zeros((R + 2 * W, W), F32)
    keep_ends(0, run(N, third, nothing))
    pass_on(z1)
    land(z1)
    tiles_mk(g_z, t_z, 4)
    a_tot, k_tot, a_z = level_mk(g_z, t_z, r_z, ae_z, z, 4)
    put_mk(g_y, y, a_tot, k_tot)
    y1 = send_part(g_y, 0, y, in_y, sem_y)
    pass_on(z2)
    land(z2)
    tiles_n(g_z, t_z, 4)
    l_tot, l_z = level_n(g_z, t_z, r_z, ae_z, z, 4)
    put_n(g_y, y, l_tot)
    y2 = send_part(g_y, 1, y, in_y, sem_y)
    keep_ends(1, run(N, fourth, nothing))
    pass_on(y1)
    land(y1)
    tiles_mk(g_y, t_y, 4)
    pass_on(y2)
    land(y2)
    tiles_n(g_y, t_y, 4)

    def level(vec, t, me, size, top=False):
        many = [zero_v, vec(0, 0)]
        for e in range(1, size - 1 if top else size):
            many.append(mm(many[e], t[e, 0]) + vec(e, 0))
        for e in range(size):
            ae[e, :R] = many[e]
        l = zero_v
        for e in reversed(range(size)):
            le[e, :R] = l
            if top and e == 0:
                break
            pushed = vec(e, 1)
            if e > 0:
                pushed = pushed + mm(many[e], t[e, 1])
            l = pushed if e == size - 1 else mm(l, t[e, 2]) + pushed
        return (many[-1], l), (ae[me, :R], le[me, :R])

    def enter(inside, r, a, l):
        return inside[0] + mm(a, r[0]), inside[1] + mm(a, r[1]) + mm(l, r[2])

    def vec_of(g):
        return lambda e, side: g[e, EH:ES] if side else g[e, EF:EN]

    def vec_small(h):
        return lambda e, side: h[e, R * side : R * side + R]

    _, (a, l) = level(vec_of(g_y), t_y, y, 4, True)
    a, l = enter((a_z, l_z), r_z, a, l)
    a, l = enter((a_c, l_c), r_c, a, l)

    def settle(v, tiles, a, l):
        for i in range(N):
            v[i] = v[i] + mm_pair(a, l, tiles[i])

    h_c[c, :R] = fh[0] + mm_pair(a, l, tfh[0])
    h_c[c, R:] = fh[1] + mm_pair(a, l, tfh[1])
    in_flight = spread(h_c, c, 2, in_c, sem_hc)
    settle(v2, tab, a, l)
    settle(v1, tab1, a, l)

    block_of = lax.broadcasted_iota(jnp.int32, (W, W), 1) // R

    def share(v, t):
        groups = [v[4 * q : 4 * q + 4].reshape(W, W) for q in range(4)]
        for dest in range(4):
            piece = groups[dest]
            for q in range(4):
                if q != dest:
                    moved = pltpu.roll(groups[q], (R * (q - dest)) % W, 1)
                    piece = jnp.where(block_of == q, moved, piece)
            ps[t, dest] = piece
        pr[t, x] = ps[t, x]
        copies = [
            pltpu.make_async_remote_copy(
                src_ref=ps.at[t, (x + j) % 4], dst_ref=pr.at[t, x],
                send_sem=sem_p.at[t, 0, j - 1], recv_sem=sem_p.at[t, 1, j - 1],
                device_id=in_x(j), device_id_type=MESH,
            )
            for j in (1, 3, 2)
        ]
        for copy in copies:
            copy.start()
        return copies

    finish(in_flight)
    (a, l), inside_c = level(vec_small(h_c), t_c, c, 2)
    h_z[z, :R] = a
    h_z[z, R:] = l
    in_flight = spread(h_z, z, 4, in_z, sem_hz)
    shared_two = share(v2, 1)
    shared_one = share(v1, 0)

    finish(states)
    edges = []
    for side, (row, where) in enumerate(((N - 1, after), (0, before))):
        for q in range(4):
            copy = pltpu.make_async_remote_copy(
                src_ref=sg.at[q, :, row], dst_ref=halo.at[side, q],
                send_sem=sem_halo.at[0, side, q], recv_sem=sem_halo.at[1, side, q],
                device_id=where, device_id_type=MESH,
            )
            copy.start()
            edges.append(copy)

    def operand(parts):
        hi, lo = split(jnp.concatenate(parts, axis=0))
        return jnp.concatenate([hi, lo], axis=1)

    def pack(i, none):
        ss[i + 1] = operand([sg[q, t, i] for t in range(2) for q in range(4)])
        return none

    run(N, pack, 0)

    finish(in_flight)
    (a, l), inside_z = level(vec_small(h_z), t_z, z, 4)
    h_y[y, :R] = a
    h_y[y, R:] = l
    in_flight = spread(h_y, y, 4, in_y, sem_hy)

    row = lax.broadcasted_iota(jnp.int32, (2 * R, 2 * W), 0)
    lane = lax.broadcasted_iota(jnp.int32, (2 * R, 2 * W), 1)
    pick = (lane == R * x + row + jnp.where(row < R, 0, W - R)).astype(F32).astype(BF16)
    by_lanes = (((1,), (1,)), ((), ()))
    for i in range(N):
        sl[i] = lax.dot_general(pick, tab[i], by_lanes, preferred_element_type=F32).astype(BF16)

    finish(edges)
    keep = ((d > 0).astype(F32), (d < 31).astype(F32))
    for side, slot in ((0, 0), (1, N + 1)):
        ss[slot] = operand([halo[side, q, t] * keep[side] for t in range(2) for q in range(4)])

    finish(in_flight)
    _, (a, l) = level(vec_small(h_y), t_y, y, 4, True)
    a, l = enter(inside_z, r_z, a, l)
    a, l = enter(inside_c, r_c, a, l)
    al[x, :, :W] = a
    al[x, :, W:] = l
    in_flight = spread(al, x, 4, in_x, sem_al)

    def turn(t):
        for sub in range(4):
            stack = jnp.concatenate(
                [pr[t, q, R * sub : R * sub + R] for q in range(4)], axis=0
            ).T
            if t == 0:
                for q in range(4):
                    base[4 * q + sub] = stack[R * q : R * q + R]
                continue
            hi, lo = split(stack)
            for q in range(4):
                lt[4 * q + sub, :R, t * W : (t + 1) * W] = hi[R * q : R * q + R]
                lt[4 * q + sub, R:, t * W : (t + 1) * W] = lo[R * q : R * q + R]

    finish(shared_two)
    turn(1)
    finish(shared_one)
    turn(0)
    finish(in_flight)
    hi, lo = split(jnp.concatenate([al[q] for q in range(4)], axis=0))
    arrived = jnp.concatenate([hi, lo], axis=0)
    for q in range(4):
        o = lax.dot_general(
            sl[4 * q : 4 * q + 4].reshape(2 * W, 2 * W), arrived, by_lanes,
            preferred_element_type=F32,
        )
        o = o[:, :W] + o[:, W:]
        for sub in range(4):
            i, low = 4 * q + sub, 2 * R * sub
            hi, lo = split(base[i] + o[low : low + R] + o[low + R : low + 2 * R])
            lt[i, :R, :W] = hi
            lt[i, R:, :W] = lo

    def grads(i, none):
        for k, j in enumerate((1, 0, 2)):
            o = jnp.dot(lt[i], ss[i + j], preferred_element_type=F32)
            o = o[:R] + o[R:]
            out_ref[k, i] = -(o[:, :W] + o[:, W:])
        return none

    run(N, grads, 0)


def body(upper_unit, lower_unit, pivot_inv, loss_grad_one, loss_grad_two, state_one, state_two):
    vmem = pl.BlockSpec(memory_space=pltpu.VMEM)
    anywhere = pl.BlockSpec(memory_space=pl.ANY)
    dma = pltpu.SemaphoreType.DMA
    tile = (2 * W, 2 * W)
    grads = pl.pallas_call(
        kernel,
        out_shape=jax.ShapeDtypeStruct((3, N, R, W), F32),
        in_specs=[anywhere] * 7,
        out_specs=vmem,
        scratch_shapes=[
            pltpu.VMEM((N, W, W), F32),
            pltpu.VMEM((N, W, W), F32),
            pltpu.VMEM((N, W, W), F32),
            pltpu.VMEM((N, R, W), F32),
            pltpu.VMEM((N, R, W), F32),
            pltpu.VMEM((N, *tile), BF16),
            pltpu.VMEM((N, *tile), BF16),
            pltpu.VMEM((N, *tile), BF16),
            pltpu.VMEM((N, *tile), BF16),
            pltpu.VMEM((N, *tile), BF16),
            pltpu.VMEM((N, R + W, W), F32),
            pltpu.VMEM((N, R + 2 * W, W), F32),
            pltpu.VMEM((N, R, W), F32),
            pltpu.VMEM((N, R, W), F32),
            pltpu.VMEM((N, R, W), F32),
            pltpu.VMEM((N, 2 * R, 2 * W), BF16),
            pltpu.VMEM((2, R, W), F32),
            pltpu.VMEM((2, *tile), BF16),
            pltpu.VMEM((4, R, 2 * W), F32),
            pltpu.VMEM((2, ES, W), F32),
            pltpu.VMEM((4, ES, W), F32),
            pltpu.VMEM((4, ES, W), F32),
            pltpu.VMEM((2, 3, *tile), BF16),
            pltpu.VMEM((4, 3, *tile), BF16),
            pltpu.VMEM((4, 3, *tile), BF16),
            pltpu.VMEM((2, 2 * R, W), F32),
            pltpu.VMEM((4, 2 * R, W), F32),
            pltpu.VMEM((4, 2 * R, W), F32),
            pltpu.VMEM((3, *tile), BF16),
            pltpu.VMEM((3, *tile), BF16),
            pltpu.VMEM((2, R + W, W), F32),
            pltpu.VMEM((4, R + W, W), F32),
            pltpu.VMEM((4, W, W), F32),
            pltpu.VMEM((4, R, W), F32),
            pltpu.VMEM((4, R + W, W), F32),
            pltpu.VMEM((4, 2, N, R, W), F32),
            pltpu.VMEM((2, 4, 2, R, W), F32),
            pltpu.VMEM((N + 2, *tile), BF16),
            pltpu.VMEM((2, 4, W, W), F32),
            pltpu.VMEM((2, 4, W, W), F32),
            pltpu.VMEM((N, 2 * R, 2 * W), BF16),
            dma((2, 2)), dma((2, 4, 3)), dma((2, 4, 3)),
            dma((2, 1)), dma((2, 3)), dma((2, 3)),
            dma((2, 3)), dma((2,)), dma((2, 2, 4)), dma((2, 2, 3)), dma((5,)), dma((2, 3)),
        ],
        compiler_params=pltpu.CompilerParams(
            collective_id=0, has_side_effects=True, vmem_limit_bytes=60 * 2**20
        ),
    )(upper_unit, lower_unit, pivot_inv, loss_grad_one, loss_grad_two, state_one, state_two)
    return jnp.transpose(grads, (2, 0, 1, 3))


def solution(mesh):
    by_rows = P("rows", None, None)
    by_both = P("rows", "rhs", None)
    return jax.shard_map(
        body,
        mesh=mesh,
        in_specs=(by_rows,) * 3 + (by_both,) * 4,
        out_specs=P("rhs", None, "rows", None),
        check_vma=False,
    )
```

```python
import jax
import jax.numpy as jnp
from jax import lax
from jax.experimental import pallas as pl
from jax.experimental.pallas import tpu as pltpu
from jax.sharding import PartitionSpec as P

MESH = pl.DeviceIdType.MESH
F32, BF16 = jnp.float32, jnp.bfloat16
N = 16
W = 128
R = 32
EM, EK, EF, EN, EH, ES = 0, 128, 256, 288, 416, 448
PARTS = ((0, EN), (EN, ES - EN))


def split(x):
    hi = x.astype(BF16)
    lo = (x - hi.astype(F32)).astype(BF16)
    return hi, lo


def tile_of(w):
    hi, lo = split(w)
    row = jnp.concatenate([hi, lo], axis=1)
    return jnp.concatenate([row, row], axis=0)


def mm(x, tile):
    hi, lo = split(x)
    both = jnp.concatenate([hi, lo], axis=1)
    out = jnp.dot(both, tile, preferred_element_type=F32)
    return out[:, :W] + out[:, W:]


def mm_pair(a, l, tile):
    ah, al = split(a)
    lh, ll = split(l)
    hi = jnp.concatenate([ah, lh], axis=1)
    lo = jnp.concatenate([al, ll], axis=1)
    out = jnp.dot(jnp.concatenate([hi, lo], axis=0), tile, preferred_element_type=F32)
    m = a.shape[0]
    out = out[:m] + out[m:]
    return out[:, :W] + out[:, W:]


def kernel(
    u_in, l_in, p_in, g1_in, g2_in, s1_ref, s2_ref, out_ref,
    u_ref, l_ref, p_ref, g1_ref, g2_ref,
    tu, tp, tl, tab, tab1, zs, zs3, v2, v1, base, sl, fh, tfh, al,
    g_c, g_z, g_y, t_c, t_z, t_y, h_c, h_z, h_y, r_c, r_z, ae_c, ae_z, ke, ae, le,
    sg, halo, ss, ps, pr, lt,
    sem_c, sem_z, sem_y, sem_hc, sem_hz, sem_hy, sem_s, sem_own, sem_halo, sem_p, sem_in, sem_al,
):
    d = lax.axis_index("rows")
    x = lax.axis_index("rhs")
    y, z, c = d // 8, (d // 2) % 4, d % 2

    def in_c(j):
        return (y * 8 + z * 2 + (c + j) % 2, x)

    def in_z(j):
        return (y * 8 + ((z + j) % 4) * 2 + c, x)

    def in_y(j):
        return (((y + j) % 4) * 8 + z * 2 + c, x)

    def in_x(j):
        return (d, (x + j) % 4)

    after, before = ((d + 1) % 32, x), ((d + 31) % 32, x)

    barrier = pltpu.get_barrier_semaphore()
    peers = [in_c(1)] + [f(j) for f in (in_z, in_y, in_x) for j in (1, 2, 3)] + [after, before]
    for peer in peers:
        pl.semaphore_signal(barrier, inc=1, device_id=peer, device_id_type=MESH)

    loads = [
        pltpu.make_async_copy(src, dst, sem_in.at[k])
        for k, (src, dst) in enumerate((
            (u_in, u_ref), (l_in, l_ref), (g2_in, g2_ref), (p_in, p_ref), (g1_in, g1_ref)
        ))
    ]
    for copy in loads:
        copy.start()
    own = [
        pltpu.make_async_copy(s, sg.at[x, t], sem_own.at[t]) for t, s in enumerate((s1_ref, s2_ref))
    ]
    for copy in own:
        copy.start()
    states = [
        pltpu.make_async_remote_copy(
            src_ref=sg.at[x], dst_ref=sg.at[x],
            send_sem=sem_s.at[0, j - 1], recv_sem=sem_s.at[1, j - 1],
            device_id=in_x(j), device_id_type=MESH,
        )
        for j in (1, 3, 2)
    ]

    def run(steps, step, carry, by=4):
        def some(b, carry):
            for s in range(by):
                carry = step(b * by + s, carry)
            return carry

        return lax.fori_loop(0, steps // by, some, carry)

    def spread(ref, me, size, where, sem):
        copies = [
            pltpu.make_async_remote_copy(
                src_ref=ref.at[me], dst_ref=ref.at[me],
                send_sem=sem.at[0, j - 1], recv_sem=sem.at[1, j - 1],
                device_id=where(j), device_id_type=MESH,
            )
            for j in range(1, size)
        ]
        for copy in copies:
            copy.start()
        return copies

    def finish(copies):
        for copy in copies:
            copy.wait()

    eye = (
        lax.broadcasted_iota(jnp.int32, (W, W), 0) == lax.broadcasted_iota(jnp.int32, (W, W), 1)
    ).astype(F32)
    zero_m = jnp.zeros((W, W), F32)
    zero_v = jnp.zeros((R, W), F32)

    def first(i, carry):
        right, left = carry
        tile, tile_p = tile_of(u_ref[i]), tile_of(p_ref[i])
        tu[i] = tile
        tp[i] = tile_p
        yv = jnp.concatenate([g2_ref[i], zero_m], axis=0) - right
        zs[i] = mm(yv, tile_p)
        k = N - 1 - i
        tile_l = tile_of(l_ref[k])
        tl[k] = tile_l
        vv = -left
        hi, lo = split(vv)
        tab[k, W:] = jnp.concatenate([hi, lo], axis=1)
        return mm(yv, tile), mm(vv, tile_l)

    for copy in loads:
        copy.wait()
    right, left = run(N, first, (jnp.concatenate([zero_v, eye], axis=0), eye))
    g_c[c, EF:EN] = right[:R]
    g_c[c, EM:EK] = right[R:]
    g_c[c, EK:EF] = left

    pl.semaphore_wait(barrier, len(peers))

    def pair(part):
        rows = pl.ds(*PARTS[part])
        copy = pltpu.make_async_remote_copy(
            src_ref=g_c.at[c, rows], dst_ref=g_c.at[c, rows],
            send_sem=sem_c.at[part, 0], recv_sem=sem_c.at[part, 1],
            device_id=in_c(1), device_id_type=MESH,
        )
        copy.start()
        return copy

    def send_part(g, part, me, where, sem):
        low, size = PARTS[part]
        rows = pl.ds(pl.multiple_of(low + c * (size // 2), 8), size // 2)
        copies, passed = [], []
        for j in range(1, 4):
            source = (me + 4 - j) % 4
            copies.append(pltpu.make_async_remote_copy(
                src_ref=g.at[me, rows], dst_ref=g.at[me, rows],
                send_sem=sem.at[part, 0, j - 1], recv_sem=sem.at[part, 1, j - 1],
                device_id=where(j), device_id_type=MESH,
            ))
            passed.append(pltpu.make_async_remote_copy(
                src_ref=g.at[source, rows], dst_ref=g.at[source, rows],
                send_sem=sem.at[part, 2, j - 1], recv_sem=sem.at[part, 3, j - 1],
                device_id=in_c(1), device_id_type=MESH,
            ))
        for j in (1, 3, 2):
            copies[j - 1].start()
        return copies, passed

    def pass_on(flight):
        copies, passed = flight
        for j in (1, 3, 2):
            copies[j - 1].wait_recv()
            passed[j - 1].start()

    def land(flight):
        copies, passed = flight
        for copy in copies:
            copy.wait_send()
        for copy in passed:
            copy.wait()

    def tiles_mk(g, t, size):
        for e in range(size):
            t[e, 0] = tile_of(g[e, EM:EK])
            t[e, 2] = tile_of(g[e, EK:EF])

    def tiles_n(g, t, size):
        for e in range(size):
            t[e, 1] = tile_of(g[e, EN:EH])

    def level_mk(g, t, kept, size):
        kept[0] = jnp.concatenate([zero_v, eye], axis=0)
        ke[size - 1] = eye
        a = jnp.concatenate([g[0, EF:EN], g[0, EM:EK]], axis=0)
        k = g[size - 1, EK:EF]
        for e in range(1, size):
            kept[e] = a
            a = mm(a, t[e, 0]) + jnp.concatenate([g[e, EF:EN], zero_m], axis=0)
            ke[size - 1 - e] = k
            k = mm(k, t[size - 1 - e, 2])
        return a, k

    def own_mk(r, kept, me):
        r[0] = tile_of(kept[me, R:])
        r[2] = tile_of(ke[me])
        return kept[me, :R]

    def level_n(g, t, kept, size):
        le[size - 1] = jnp.concatenate([zero_v, zero_m], axis=0)
        for e in reversed(range(size)):
            source = jnp.concatenate([g[e, EH:ES], zero_m], axis=0)
            if e == 0:
                pushed = source + jnp.concatenate([zero_v, g[0, EN:EH]], axis=0)
            else:
                pushed = source + mm(kept[e], t[e, 1])
            l = pushed if e == size - 1 else mm(l, t[e, 2]) + pushed
            if e > 0:
                le[e - 1] = l
        return l

    def own_n(r, me):
        r[1] = tile_of(le[me, R:])
        return le[me, :R]

    def put_mk(g, me, a, k):
        g[me, EF:EN] = a[:R]
        g[me, EM:EK] = a[R:]
        g[me, EK:EF] = k

    def put_n(g, me, l):
        g[me, EH:ES] = l[:R]
        g[me, EN:EH] = l[R:]

    def second(k, carry):
        i = N - 1 - k
        vv = zs[i] - carry
        v2[i] = vv[:R]
        hi, lo = split(vv[R:])
        tab[i, :W] = jnp.concatenate([hi, lo], axis=1)
        return mm(vv, tl[i])

    c1 = pair(0)
    for copy in own:
        copy.wait()
    for copy in states:
        copy.start()
    carry = run(N // 2, second, jnp.concatenate([zero_v, zero_m], axis=0))
    c1.wait()
    tiles_mk(g_c, t_c, 2)
    a_tot, k_tot = level_mk(g_c, t_c, ae_c, 2)
    put_mk(g_z, z, a_tot, k_tot)
    z1 = send_part(g_z, 0, z, in_z, sem_z)
    a_c = own_mk(r_c, ae_c, c)
    carry = run(N // 2, lambda k, v: second(k + N // 2, v), carry)
    put_n(g_c, c, carry)
    c2 = pair(1)
    c2.wait()
    tiles_n(g_c, t_c, 2)
    l_tot = level_n(g_c, t_c, ae_c, 2)
    put_n(g_z, z, l_tot)
    z2 = send_part(g_z, 1, z, in_z, sem_z)
    l_c = own_n(r_c, c)

    def third(i, carry):
        responses = tab[i, :, :W].astype(F32) + tab[i, :, W:].astype(F32)
        yv = jnp.concatenate([g1_ref[i] + v2[i], responses], axis=0) - carry
        zs3[i] = mm(yv, tp[i])
        return mm(yv, tu[i])

    def fourth(k, carry):
        i = N - 1 - k
        vv = zs3[i] - carry
        v1[i] = vv[:R]
        hi, lo = split(vv[R:])
        tab1[i] = jnp.concatenate([hi, lo], axis=1)
        return mm(vv, tl[i])

    def keep_ends(side, carry):
        fh[side] = carry[:R]
        hi, lo = split(carry[R:])
        tfh[side] = jnp.concatenate([hi, lo], axis=1)

    nothing = jnp.zeros((R + 2 * W, W), F32)
    keep_ends(0, run(N, third, nothing))
    pass_on(z1)
    land(z1)
    tiles_mk(g_z, t_z, 4)
    a_tot, k_tot = level_mk(g_z, t_z, ae_z, 4)
    put_mk(g_y, y, a_tot, k_tot)
    y1 = send_part(g_y, 0, y, in_y, sem_y)
    a_z = own_mk(r_z, ae_z, z)
    pass_on(z2)
    land(z2)
    tiles_n(g_z, t_z, 4)
    l_tot = level_n(g_z, t_z, ae_z, 4)
    put_n(g_y, y, l_tot)
    y2 = send_part(g_y, 1, y, in_y, sem_y)
    l_z = own_n(r_z, z)
    keep_ends(1, run(N, fourth, nothing))

    row = lax.broadcasted_iota(jnp.int32, (2 * R, 2 * W), 0)
    lane = lax.broadcasted_iota(jnp.int32, (2 * R, 2 * W), 1)
    pick = (lane == R * x + row + jnp.where(row < R, 0, W - R)).astype(F32).astype(BF16)
    by_lanes = (((1,), (1,)), ((), ()))
    for i in range(N):
        sl[i] = lax.dot_general(pick, tab[i], by_lanes, preferred_element_type=F32).astype(BF16)

    pass_on(y1)
    land(y1)
    tiles_mk(g_y, t_y, 4)
    pass_on(y2)
    land(y2)
    tiles_n(g_y, t_y, 4)

    def level(vec, t, me, size, top=False):
        many = [zero_v, vec(0, 0)]
        for e in range(1, size - 1 if top else size):
            many.append(mm(many[e], t[e, 0]) + vec(e, 0))
        for e in range(size):
            ae[e, :R] = many[e]
        l = zero_v
        for e in reversed(range(size)):
            le[e, :R] = l
            if top and e == 0:
                break
            pushed = vec(e, 1)
            if e > 0:
                pushed = pushed + mm(many[e], t[e, 1])
            l = pushed if e == size - 1 else mm(l, t[e, 2]) + pushed
        return (many[-1], l), (ae[me, :R], le[me, :R])

    def enter(inside, r, a, l):
        return inside[0] + mm(a, r[0]), inside[1] + mm(a, r[1]) + mm(l, r[2])

    def vec_of(g):
        return lambda e, side: g[e, EH:ES] if side else g[e, EF:EN]

    def vec_small(h):
        return lambda e, side: h[e, R * side : R * side + R]

    _, (a, l) = level(vec_of(g_y), t_y, y, 4, True)
    a, l = enter((a_z, l_z), r_z, a, l)
    a, l = enter((a_c, l_c), r_c, a, l)

    def settle(v, tiles, a, l):
        for i in range(N):
            v[i] = v[i] + mm_pair(a, l, tiles[i])

    h_c[c, :R] = fh[0] + mm_pair(a, l, tfh[0])
    h_c[c, R:] = fh[1] + mm_pair(a, l, tfh[1])
    in_flight = spread(h_c, c, 2, in_c, sem_hc)
    settle(v2, tab, a, l)
    settle(v1, tab1, a, l)

    block_of = lax.broadcasted_iota(jnp.int32, (W, W), 1) // R

    def share(v, t):
        groups = [v[4 * q : 4 * q + 4].reshape(W, W) for q in range(4)]
        for dest in range(4):
            piece = groups[dest]
            for q in range(4):
                if q != dest:
                    moved = pltpu.roll(groups[q], (R * (q - dest)) % W, 1)
                    piece = jnp.where(block_of == q, moved, piece)
            ps[t, dest] = piece
        pr[t, x] = ps[t, x]
        copies = [
            pltpu.make_async_remote_copy(
                src_ref=ps.at[t, (x + j) % 4], dst_ref=pr.at[t, x],
                send_sem=sem_p.at[t, 0, j - 1], recv_sem=sem_p.at[t, 1, j - 1],
                device_id=in_x(j), device_id_type=MESH,
            )
            for j in (1, 3, 2)
        ]
        for copy in copies:
            copy.start()
        return copies

    finish(in_flight)
    (a, l), inside_c = level(vec_small(h_c), t_c, c, 2)
    h_z[z, :R] = a
    h_z[z, R:] = l
    in_flight = spread(h_z, z, 4, in_z, sem_hz)
    shared_two = share(v2, 1)
    shared_one = share(v1, 0)

    finish(in_flight)
    (a, l), inside_z = level(vec_small(h_z), t_z, z, 4)
    h_y[y, :R] = a
    h_y[y, R:] = l
    in_flight = spread(h_y, y, 4, in_y, sem_hy)

    finish(states)
    edges = []
    for side, (row, where) in enumerate(((N - 1, after), (0, before))):
        for q in range(4):
            copy = pltpu.make_async_remote_copy(
                src_ref=sg.at[q, :, row], dst_ref=halo.at[side, q],
                send_sem=sem_halo.at[0, side, q], recv_sem=sem_halo.at[1, side, q],
                device_id=where, device_id_type=MESH,
            )
            copy.start()
            edges.append(copy)

    def operand(parts):
        hi, lo = split(jnp.concatenate(parts, axis=0))
        return jnp.concatenate([hi, lo], axis=1)

    def pack(i, none):
        ss[i + 1] = operand([sg[q, t, i] for t in range(2) for q in range(4)])
        return none

    run(N, pack, 0)

    finish(in_flight)
    _, (a, l) = level(vec_small(h_y), t_y, y, 4, True)
    a, l = enter(inside_z, r_z, a, l)
    a, l = enter(inside_c, r_c, a, l)
    al[x, :, :W] = a
    al[x, :, W:] = l
    in_flight = spread(al, x, 4, in_x, sem_al)

    def turn(t):
        for sub in range(4):
            stack = jnp.concatenate(
                [pr[t, q, R * sub : R * sub + R] for q in range(4)], axis=0
            ).T
            if t == 0:
                for q in range(4):
                    base[4 * q + sub] = stack[R * q : R * q + R]
                continue
            hi, lo = split(stack)
            for q in range(4):
                lt[4 * q + sub, :R, t * W : (t + 1) * W] = hi[R * q : R * q + R]
                lt[4 * q + sub, R:, t * W : (t + 1) * W] = lo[R * q : R * q + R]

    finish(shared_two)
    turn(1)
    finish(shared_one)
    turn(0)
    finish(edges)
    keep = ((d > 0).astype(F32), (d < 31).astype(F32))
    for side, slot in ((0, 0), (1, N + 1)):
        ss[slot] = operand([halo[side, q, t] * keep[side] for t in range(2) for q in range(4)])
    finish(in_flight)
    hi, lo = split(jnp.concatenate([al[q] for q in range(4)], axis=0))
    arrived = jnp.concatenate([hi, lo], axis=0)
    for q in range(4):
        o = lax.dot_general(
            sl[4 * q : 4 * q + 4].reshape(2 * W, 2 * W), arrived, by_lanes,
            preferred_element_type=F32,
        )
        o = o[:, :W] + o[:, W:]
        for sub in range(4):
            i, low = 4 * q + sub, 2 * R * sub
            hi, lo = split(base[i] + o[low : low + R] + o[low + R : low + 2 * R])
            lt[i, :R, :W] = hi
            lt[i, R:, :W] = lo

    for j in range(N + 2):
        low, high = max(j - 2, 0), min(j + 1, N)
        o = jnp.dot(
            lt[low:high].reshape(2 * R * (high - low), 2 * W), ss[j], preferred_element_type=F32
        )
        o = o[:, :W] + o[:, W:]
        for i in range(low, high):
            at = 2 * R * (i - low)
            out_ref[(1, 0, 2)[j - i], i] = -(o[at : at + R] + o[at + R : at + 2 * R])


def body(upper_unit, lower_unit, pivot_inv, loss_grad_one, loss_grad_two, state_one, state_two):
    vmem = pl.BlockSpec(memory_space=pltpu.VMEM)
    anywhere = pl.BlockSpec(memory_space=pltpu.HBM)
    dma = pltpu.SemaphoreType.DMA
    tile = (2 * W, 2 * W)
    grads = pl.pallas_call(
        kernel,
        out_shape=pltpu.VMEM((3, N, R, W), F32),
        in_specs=[anywhere] * 7,
        out_specs=vmem,
        scratch_shapes=[
            pltpu.VMEM((N, W, W), F32),
            pltpu.VMEM((N, W, W), F32),
            pltpu.VMEM((N, W, W), F32),
            pltpu.VMEM((N, R, W), F32),
            pltpu.VMEM((N, R, W), F32),
            pltpu.VMEM((N, *tile), BF16),
            pltpu.VMEM((N, *tile), BF16),
            pltpu.VMEM((N, *tile), BF16),
            pltpu.VMEM((N, *tile), BF16),
            pltpu.VMEM((N, *tile), BF16),
            pltpu.VMEM((N, R + W, W), F32),
            pltpu.VMEM((N, R + 2 * W, W), F32),
            pltpu.VMEM((N, R, W), F32),
            pltpu.VMEM((N, R, W), F32),
            pltpu.VMEM((N, R, W), F32),
            pltpu.VMEM((N, 2 * R, 2 * W), BF16),
            pltpu.VMEM((2, R, W), F32),
            pltpu.VMEM((2, *tile), BF16),
            pltpu.VMEM((4, R, 2 * W), F32),
            pltpu.VMEM((2, ES, W), F32),
            pltpu.VMEM((4, ES, W), F32),
            pltpu.VMEM((4, ES, W), F32),
            pltpu.VMEM((2, 3, *tile), BF16),
            pltpu.VMEM((4, 3, *tile), BF16),
            pltpu.VMEM((4, 3, *tile), BF16),
            pltpu.VMEM((2, 2 * R, W), F32),
            pltpu.VMEM((4, 2 * R, W), F32),
            pltpu.VMEM((4, 2 * R, W), F32),
            pltpu.VMEM((3, *tile), BF16),
            pltpu.VMEM((3, *tile), BF16),
            pltpu.VMEM((2, R + W, W), F32),
            pltpu.VMEM((4, R + W, W), F32),
            pltpu.VMEM((4, W, W), F32),
            pltpu.VMEM((4, R, W), F32),
            pltpu.VMEM((4, R + W, W), F32),
            pltpu.VMEM((4, 2, N, R, W), F32),
            pltpu.VMEM((2, 4, 2, R, W), F32),
            pltpu.VMEM((N + 2, *tile), BF16),
            pltpu.VMEM((2, 4, W, W), F32),
            pltpu.VMEM((2, 4, W, W), F32),
            pltpu.VMEM((N, 2 * R, 2 * W), BF16),
            dma((2, 2)), dma((2, 4, 3)), dma((2, 4, 3)),
            dma((2, 1)), dma((2, 3)), dma((2, 3)),
            dma((2, 3)), dma((2,)), dma((2, 2, 4)), dma((2, 2, 3)), dma((5,)), dma((2, 3)),
        ],
        compiler_params=pltpu.CompilerParams(
            collective_id=0, has_side_effects=True, vmem_limit_bytes=66_200_000
        ),
    )(upper_unit, lower_unit, pivot_inv, loss_grad_one, loss_grad_two, state_one, state_two)
    return jnp.transpose(grads, (2, 0, 1, 3))


def solution(mesh):
    by_rows = P("rows", None, None)
    by_both = P("rows", "rhs", None)
    return jax.shard_map(
        body,
        mesh=mesh,
        in_specs=(by_rows,) * 3 + (by_both,) * 4,
        out_specs=P("rhs", None, "rows", None),
        check_vma=False,
    )
```

```python
import jax
import jax.numpy as jnp
from jax import lax
from jax.experimental import pallas as pl
from jax.experimental.pallas import tpu as pltpu
from jax.sharding import PartitionSpec as P

MESH = pl.DeviceIdType.MESH
F32, BF16 = jnp.float32, jnp.bfloat16
N = 16
W = 128
R = 32
EM, EK, EF, EN, EH, ES = 0, 128, 256, 288, 416, 448
PARTS = ((0, EN), (EN, ES - EN))


def split(x):
    hi = x.astype(BF16)
    lo = (x - hi.astype(F32)).astype(BF16)
    return hi, lo


def tile_of(w):
    hi, lo = split(w)
    row = jnp.concatenate([hi, lo], axis=1)
    return jnp.concatenate([row, row], axis=0)


def mm(x, tile):
    hi, lo = split(x)
    both = jnp.concatenate([hi, lo], axis=1)
    out = jnp.dot(both, tile, preferred_element_type=F32)
    return out[:, :W] + out[:, W:]


def mm_pair(a, l, tile):
    ah, al = split(a)
    lh, ll = split(l)
    hi = jnp.concatenate([ah, lh], axis=1)
    lo = jnp.concatenate([al, ll], axis=1)
    out = jnp.dot(jnp.concatenate([hi, lo], axis=0), tile, preferred_element_type=F32)
    m = a.shape[0]
    out = out[:m] + out[m:]
    return out[:, :W] + out[:, W:]


def kernel(
    u_in, l_in, p_in, g1_in, g2_in, s1_ref, s2_ref, out_ref,
    u_ref, l_ref, p_ref, g1_ref, g2_ref,
    tu, tp, tl, tab, tab1, zs, zs3, v2, v1, base, sl, fh, tfh, al,
    g_c, g_z, g_y, t_c, t_z, t_y, h_c, h_z, h_y, r_c, r_z, ae_c, ae_z, ke, ae, le,
    sg, halo, ss, ps, pr, lt,
    sem_c, sem_z, sem_y, sem_hc, sem_hz, sem_hy, sem_s, sem_own, sem_halo, sem_p, sem_in, sem_al,
):
    d = lax.axis_index("rows")
    x = lax.axis_index("rhs")
    y, z, c = d // 8, (d // 2) % 4, d % 2

    def in_c(j):
        return (y * 8 + z * 2 + (c + j) % 2, x)

    def in_z(j):
        return (y * 8 + ((z + j) % 4) * 2 + c, x)

    def in_y(j):
        return (((y + j) % 4) * 8 + z * 2 + c, x)

    def in_x(j):
        return (d, (x + j) % 4)

    after, before = ((d + 1) % 32, x), ((d + 31) % 32, x)

    barrier = pltpu.get_barrier_semaphore()
    peers = [in_c(1)] + [f(j) for f in (in_z, in_y, in_x) for j in (1, 2, 3)] + [after, before]
    for peer in peers:
        pl.semaphore_signal(barrier, inc=1, device_id=peer, device_id_type=MESH)

    loads = [
        pltpu.make_async_copy(src, dst, sem_in.at[k])
        for k, (src, dst) in enumerate((
            (u_in, u_ref), (l_in, l_ref), (g2_in, g2_ref), (p_in, p_ref), (g1_in, g1_ref)
        ))
    ]
    for copy in loads:
        copy.start()
    own = [
        pltpu.make_async_copy(s, sg.at[x, t], sem_own.at[t]) for t, s in enumerate((s1_ref, s2_ref))
    ]
    for copy in own:
        copy.start()
    states = [
        pltpu.make_async_remote_copy(
            src_ref=sg.at[x], dst_ref=sg.at[x],
            send_sem=sem_s.at[0, j - 1], recv_sem=sem_s.at[1, j - 1],
            device_id=in_x(j), device_id_type=MESH,
        )
        for j in (1, 3, 2)
    ]

    def run(steps, step, carry, by=4):
        def some(b, carry):
            for s in range(by):
                carry = step(b * by + s, carry)
            return carry

        return lax.fori_loop(0, steps // by, some, carry)

    def spread(ref, me, size, where, sem):
        copies = [
            pltpu.make_async_remote_copy(
                src_ref=ref.at[me], dst_ref=ref.at[me],
                send_sem=sem.at[0, j - 1], recv_sem=sem.at[1, j - 1],
                device_id=where(j), device_id_type=MESH,
            )
            for j in range(1, size)
        ]
        for copy in copies:
            copy.start()
        return copies

    sent = []

    def finish(copies):
        for copy in copies:
            copy.wait_recv()
        sent.extend(copies)

    eye = (
        lax.broadcasted_iota(jnp.int32, (W, W), 0) == lax.broadcasted_iota(jnp.int32, (W, W), 1)
    ).astype(F32)
    zero_m = jnp.zeros((W, W), F32)
    zero_v = jnp.zeros((R, W), F32)

    def first(i, carry):
        right, left = carry
        tile, tile_p = tile_of(u_ref[i]), tile_of(p_ref[i])
        tu[i] = tile
        tp[i] = tile_p
        yv = jnp.concatenate([g2_ref[i], zero_m], axis=0) - right
        zs[i] = mm(yv, tile_p)
        k = N - 1 - i
        tile_l = tile_of(l_ref[k])
        tl[k] = tile_l
        vv = -left
        hi, lo = split(vv)
        tab[k, W:] = jnp.concatenate([hi, lo], axis=1)
        return mm(yv, tile), mm(vv, tile_l)

    for copy in loads:
        copy.wait()
    right, left = run(N, first, (jnp.concatenate([zero_v, eye], axis=0), eye))
    g_c[c, EF:EN] = right[:R]
    g_c[c, EM:EK] = right[R:]
    g_c[c, EK:EF] = left

    pl.semaphore_wait(barrier, len(peers))

    def pair(part):
        rows = pl.ds(*PARTS[part])
        copy = pltpu.make_async_remote_copy(
            src_ref=g_c.at[c, rows], dst_ref=g_c.at[c, rows],
            send_sem=sem_c.at[part, 0], recv_sem=sem_c.at[part, 1],
            device_id=in_c(1), device_id_type=MESH,
        )
        copy.start()
        return copy

    def send_part(g, part, me, where, sem):
        low, size = PARTS[part]
        rows = pl.ds(pl.multiple_of(low + c * (size // 2), 8), size // 2)
        copies, passed = [], []
        for j in range(1, 4):
            source = (me + 4 - j) % 4
            copies.append(pltpu.make_async_remote_copy(
                src_ref=g.at[me, rows], dst_ref=g.at[me, rows],
                send_sem=sem.at[part, 0, j - 1], recv_sem=sem.at[part, 1, j - 1],
                device_id=where(j), device_id_type=MESH,
            ))
            passed.append(pltpu.make_async_remote_copy(
                src_ref=g.at[source, rows], dst_ref=g.at[source, rows],
                send_sem=sem.at[part, 2, j - 1], recv_sem=sem.at[part, 3, j - 1],
                device_id=in_c(1), device_id_type=MESH,
            ))
        for j in (1, 3, 2):
            copies[j - 1].start()
        return copies, passed

    def pass_on(flight):
        copies, passed = flight
        for j in (1, 3, 2):
            copies[j - 1].wait_recv()
            passed[j - 1].start()

    def land(flight):
        copies, passed = flight
        for copy in passed:
            copy.wait_recv()
        sent.extend(copies + passed)

    def tiles_mk(g, t, size):
        for e in range(size):
            t[e, 0] = tile_of(g[e, EM:EK])
            t[e, 2] = tile_of(g[e, EK:EF])

    def tiles_n(g, t, size):
        for e in range(size):
            t[e, 1] = tile_of(g[e, EN:EH])

    def level_mk(g, t, kept, size):
        kept[0] = jnp.concatenate([zero_v, eye], axis=0)
        ke[size - 1] = eye
        a = jnp.concatenate([g[0, EF:EN], g[0, EM:EK]], axis=0)
        k = g[size - 1, EK:EF]
        for e in range(1, size):
            kept[e] = a
            a = mm(a, t[e, 0]) + jnp.concatenate([g[e, EF:EN], zero_m], axis=0)
            ke[size - 1 - e] = k
            k = mm(k, t[size - 1 - e, 2])
        return a, k

    def own_mk(r, kept, me):
        r[0] = tile_of(kept[me, R:])
        r[2] = tile_of(ke[me])
        return kept[me, :R]

    def level_n(g, t, kept, size):
        le[size - 1] = jnp.concatenate([zero_v, zero_m], axis=0)
        for e in reversed(range(size)):
            source = jnp.concatenate([g[e, EH:ES], zero_m], axis=0)
            if e == 0:
                pushed = source + jnp.concatenate([zero_v, g[0, EN:EH]], axis=0)
            else:
                pushed = source + mm(kept[e], t[e, 1])
            l = pushed if e == size - 1 else mm(l, t[e, 2]) + pushed
            if e > 0:
                le[e - 1] = l
        return l

    def own_n(r, me):
        r[1] = tile_of(le[me, R:])
        return le[me, :R]

    def put_mk(g, me, a, k):
        g[me, EF:EN] = a[:R]
        g[me, EM:EK] = a[R:]
        g[me, EK:EF] = k

    def put_n(g, me, l):
        g[me, EH:ES] = l[:R]
        g[me, EN:EH] = l[R:]

    def second(k, carry):
        i = N - 1 - k
        vv = zs[i] - carry
        v2[i] = vv[:R]
        hi, lo = split(vv[R:])
        tab[i, :W] = jnp.concatenate([hi, lo], axis=1)
        return mm(vv, tl[i])

    c1 = pair(0)
    for copy in own:
        copy.wait()
    for copy in states:
        copy.start()
    carry = run(N // 2, second, jnp.concatenate([zero_v, zero_m], axis=0))
    finish([c1])
    tiles_mk(g_c, t_c, 2)
    a_tot, k_tot = level_mk(g_c, t_c, ae_c, 2)
    put_mk(g_z, z, a_tot, k_tot)
    z1 = send_part(g_z, 0, z, in_z, sem_z)
    a_c = own_mk(r_c, ae_c, c)
    carry = run(N // 2, lambda k, v: second(k + N // 2, v), carry)
    put_n(g_c, c, carry)
    c2 = pair(1)
    finish([c2])
    tiles_n(g_c, t_c, 2)
    l_tot = level_n(g_c, t_c, ae_c, 2)
    put_n(g_z, z, l_tot)
    z2 = send_part(g_z, 1, z, in_z, sem_z)
    l_c = own_n(r_c, c)

    def third(i, carry):
        responses = tab[i, :, :W].astype(F32) + tab[i, :, W:].astype(F32)
        yv = jnp.concatenate([g1_ref[i] + v2[i], responses], axis=0) - carry
        zs3[i] = mm(yv, tp[i])
        return mm(yv, tu[i])

    def fourth(k, carry):
        i = N - 1 - k
        vv = zs3[i] - carry
        v1[i] = vv[:R]
        hi, lo = split(vv[R:])
        tab1[i] = jnp.concatenate([hi, lo], axis=1)
        return mm(vv, tl[i])

    def keep_ends(side, carry):
        fh[side] = carry[:R]
        hi, lo = split(carry[R:])
        tfh[side] = jnp.concatenate([hi, lo], axis=1)

    nothing = jnp.zeros((R + 2 * W, W), F32)
    keep_ends(0, run(N, third, nothing))
    pass_on(z1)
    land(z1)
    tiles_mk(g_z, t_z, 4)
    a_tot, k_tot = level_mk(g_z, t_z, ae_z, 4)
    put_mk(g_y, y, a_tot, k_tot)
    y1 = send_part(g_y, 0, y, in_y, sem_y)
    a_z = own_mk(r_z, ae_z, z)
    pass_on(z2)
    land(z2)
    tiles_n(g_z, t_z, 4)
    l_tot = level_n(g_z, t_z, ae_z, 4)
    put_n(g_y, y, l_tot)
    y2 = send_part(g_y, 1, y, in_y, sem_y)
    l_z = own_n(r_z, z)
    keep_ends(1, run(N, fourth, nothing))

    row = lax.broadcasted_iota(jnp.int32, (2 * R, 2 * W), 0)
    lane = lax.broadcasted_iota(jnp.int32, (2 * R, 2 * W), 1)
    pick = (lane == R * x + row + jnp.where(row < R, 0, W - R)).astype(F32).astype(BF16)
    by_lanes = (((1,), (1,)), ((), ()))
    for i in range(N):
        sl[i] = lax.dot_general(pick, tab[i], by_lanes, preferred_element_type=F32).astype(BF16)

    pass_on(y1)
    land(y1)
    tiles_mk(g_y, t_y, 4)
    pass_on(y2)
    land(y2)
    tiles_n(g_y, t_y, 4)

    def level(vec, t, me, size, top=False):
        many = [zero_v, vec(0, 0)]
        for e in range(1, size - 1 if top else size):
            many.append(mm(many[e], t[e, 0]) + vec(e, 0))
        for e in range(size):
            ae[e, :R] = many[e]
        l = zero_v
        for e in reversed(range(size)):
            le[e, :R] = l
            if top and e == 0:
                break
            pushed = vec(e, 1)
            if e > 0:
                pushed = pushed + mm(many[e], t[e, 1])
            l = pushed if e == size - 1 else mm(l, t[e, 2]) + pushed
        return (many[-1], l), (ae[me, :R], le[me, :R])

    def enter(inside, r, a, l):
        return inside[0] + mm(a, r[0]), inside[1] + mm(a, r[1]) + mm(l, r[2])

    def vec_of(g):
        return lambda e, side: g[e, EH:ES] if side else g[e, EF:EN]

    def vec_small(h):
        return lambda e, side: h[e, R * side : R * side + R]

    _, (a, l) = level(vec_of(g_y), t_y, y, 4, True)
    a, l = enter((a_z, l_z), r_z, a, l)
    a, l = enter((a_c, l_c), r_c, a, l)

    def settle(v, tiles, a, l):
        for i in range(N):
            v[i] = v[i] + mm_pair(a, l, tiles[i])

    h_c[c, :R] = fh[0] + mm_pair(a, l, tfh[0])
    h_c[c, R:] = fh[1] + mm_pair(a, l, tfh[1])
    in_flight = spread(h_c, c, 2, in_c, sem_hc)
    settle(v2, tab, a, l)
    settle(v1, tab1, a, l)

    block_of = lax.broadcasted_iota(jnp.int32, (W, W), 1) // R

    def share(v, t):
        groups = [v[4 * q : 4 * q + 4].reshape(W, W) for q in range(4)]
        for dest in range(4):
            piece = groups[dest]
            for q in range(4):
                if q != dest:
                    moved = pltpu.roll(groups[q], (R * (q - dest)) % W, 1)
                    piece = jnp.where(block_of == q, moved, piece)
            ps[t, dest] = piece
        pr[t, x] = ps[t, x]
        copies = [
            pltpu.make_async_remote_copy(
                src_ref=ps.at[t, (x + j) % 4], dst_ref=pr.at[t, x],
                send_sem=sem_p.at[t, 0, j - 1], recv_sem=sem_p.at[t, 1, j - 1],
                device_id=in_x(j), device_id_type=MESH,
            )
            for j in (1, 3, 2)
        ]
        for copy in copies:
            copy.start()
        return copies

    finish(in_flight)
    (a, l), inside_c = level(vec_small(h_c), t_c, c, 2)
    h_z[z, :R] = a
    h_z[z, R:] = l
    in_flight = spread(h_z, z, 4, in_z, sem_hz)
    shared_two = share(v2, 1)
    shared_one = share(v1, 0)

    finish(in_flight)
    (a, l), inside_z = level(vec_small(h_z), t_z, z, 4)
    h_y[y, :R] = a
    h_y[y, R:] = l
    in_flight = spread(h_y, y, 4, in_y, sem_hy)

    finish(states)
    edges = []
    for side, (row, where) in enumerate(((N - 1, after), (0, before))):
        for q in range(4):
            copy = pltpu.make_async_remote_copy(
                src_ref=sg.at[q, :, row], dst_ref=halo.at[side, q],
                send_sem=sem_halo.at[0, side, q], recv_sem=sem_halo.at[1, side, q],
                device_id=where, device_id_type=MESH,
            )
            copy.start()
            edges.append(copy)

    def operand(parts):
        hi, lo = split(jnp.concatenate(parts, axis=0))
        return jnp.concatenate([hi, lo], axis=1)

    def pack(i, none):
        ss[i + 1] = operand([sg[q, t, i] for t in range(2) for q in range(4)])
        return none

    run(N, pack, 0)

    finish(in_flight)
    _, (a, l) = level(vec_small(h_y), t_y, y, 4, True)
    a, l = enter(inside_z, r_z, a, l)
    a, l = enter(inside_c, r_c, a, l)
    al[x, :, :W] = a
    al[x, :, W:] = l
    in_flight = spread(al, x, 4, in_x, sem_al)

    def turn(t):
        for sub in range(4):
            stack = jnp.concatenate(
                [pr[t, q, R * sub : R * sub + R] for q in range(4)], axis=0
            ).T
            if t == 0:
                for q in range(4):
                    base[4 * q + sub] = stack[R * q : R * q + R]
                continue
            hi, lo = split(stack)
            for q in range(4):
                lt[4 * q + sub, :R, t * W : (t + 1) * W] = hi[R * q : R * q + R]
                lt[4 * q + sub, R:, t * W : (t + 1) * W] = lo[R * q : R * q + R]

    finish(shared_two)
    turn(1)
    finish(shared_one)
    turn(0)
    finish(edges)
    keep = ((d > 0).astype(F32), (d < 31).astype(F32))
    for side, slot in ((0, 0), (1, N + 1)):
        ss[slot] = operand([halo[side, q, t] * keep[side] for t in range(2) for q in range(4)])
    finish(in_flight)
    hi, lo = split(jnp.concatenate([al[q] for q in range(4)], axis=0))
    arrived = jnp.concatenate([hi, lo], axis=0)
    for q in range(4):
        o = lax.dot_general(
            sl[4 * q : 4 * q + 4].reshape(2 * W, 2 * W), arrived, by_lanes,
            preferred_element_type=F32,
        )
        o = o[:, :W] + o[:, W:]
        for sub in range(4):
            i, low = 4 * q + sub, 2 * R * sub
            hi, lo = split(base[i] + o[low : low + R] + o[low + R : low + 2 * R])
            lt[i, :R, :W] = hi
            lt[i, R:, :W] = lo

    for j in range(N + 2):
        low, high = max(j - 2, 0), min(j + 1, N)
        o = jnp.dot(
            lt[low:high].reshape(2 * R * (high - low), 2 * W), ss[j], preferred_element_type=F32
        )
        o = o[:, :W] + o[:, W:]
        for i in range(low, high):
            at = 2 * R * (i - low)
            out_ref[(1, 0, 2)[j - i], i] = -(o[at : at + R] + o[at + R : at + 2 * R])

    for copy in sent:
        copy.wait_send()


def body(upper_unit, lower_unit, pivot_inv, loss_grad_one, loss_grad_two, state_one, state_two):
    vmem = pl.BlockSpec(memory_space=pltpu.VMEM)
    anywhere = pl.BlockSpec(memory_space=pltpu.HBM)
    dma = pltpu.SemaphoreType.DMA
    tile = (2 * W, 2 * W)
    grads = pl.pallas_call(
        kernel,
        out_shape=pltpu.VMEM((3, N, R, W), F32),
        in_specs=[anywhere] * 7,
        out_specs=vmem,
        scratch_shapes=[
            pltpu.VMEM((N, W, W), F32),
            pltpu.VMEM((N, W, W), F32),
            pltpu.VMEM((N, W, W), F32),
            pltpu.VMEM((N, R, W), F32),
            pltpu.VMEM((N, R, W), F32),
            pltpu.VMEM((N, *tile), BF16),
            pltpu.VMEM((N, *tile), BF16),
            pltpu.VMEM((N, *tile), BF16),
            pltpu.VMEM((N, *tile), BF16),
            pltpu.VMEM((N, *tile), BF16),
            pltpu.VMEM((N, R + W, W), F32),
            pltpu.VMEM((N, R + 2 * W, W), F32),
            pltpu.VMEM((N, R, W), F32),
            pltpu.VMEM((N, R, W), F32),
            pltpu.VMEM((N, R, W), F32),
            pltpu.VMEM((N, 2 * R, 2 * W), BF16),
            pltpu.VMEM((2, R, W), F32),
            pltpu.VMEM((2, *tile), BF16),
            pltpu.VMEM((4, R, 2 * W), F32),
            pltpu.VMEM((2, ES, W), F32),
            pltpu.VMEM((4, ES, W), F32),
            pltpu.VMEM((4, ES, W), F32),
            pltpu.VMEM((2, 3, *tile), BF16),
            pltpu.VMEM((4, 3, *tile), BF16),
            pltpu.VMEM((4, 3, *tile), BF16),
            pltpu.VMEM((2, 2 * R, W), F32),
            pltpu.VMEM((4, 2 * R, W), F32),
            pltpu.VMEM((4, 2 * R, W), F32),
            pltpu.VMEM((3, *tile), BF16),
            pltpu.VMEM((3, *tile), BF16),
            pltpu.VMEM((2, R + W, W), F32),
            pltpu.VMEM((4, R + W, W), F32),
            pltpu.VMEM((4, W, W), F32),
            pltpu.VMEM((4, R, W), F32),
            pltpu.VMEM((4, R + W, W), F32),
            pltpu.VMEM((4, 2, N, R, W), F32),
            pltpu.VMEM((2, 4, 2, R, W), F32),
            pltpu.VMEM((N + 2, *tile), BF16),
            pltpu.VMEM((2, 4, W, W), F32),
            pltpu.VMEM((2, 4, W, W), F32),
            pltpu.VMEM((N, 2 * R, 2 * W), BF16),
            dma((2, 2)), dma((2, 4, 3)), dma((2, 4, 3)),
            dma((2, 1)), dma((2, 3)), dma((2, 3)),
            dma((2, 3)), dma((2,)), dma((2, 2, 4)), dma((2, 2, 3)), dma((5,)), dma((2, 3)),
        ],
        compiler_params=pltpu.CompilerParams(
            collective_id=0, has_side_effects=True, vmem_limit_bytes=66_200_000
        ),
    )(upper_unit, lower_unit, pivot_inv, loss_grad_one, loss_grad_two, state_one, state_two)
    return jnp.transpose(grads, (2, 0, 1, 3))


def solution(mesh):
    by_rows = P("rows", None, None)
    by_both = P("rows", "rhs", None)
    return jax.shard_map(
        body,
        mesh=mesh,
        in_specs=(by_rows,) * 3 + (by_both,) * 4,
        out_specs=P("rhs", None, "rows", None),
        check_vma=False,
    )
```
